8 devices in a mesh: rep: 2 (over z, y), rows: 4 (over x, core).
Axes of the slice: x: 2, y: 2, z: 1, core: 2. Of those that a mesh axis runs over, the one named last changes fastest.
Arguments:
- adjacency: bfloat16 [8192, 8192], P('rows', 'rep')
- features: bfloat16 [8192, 100], P('rows')
- w_one: bfloat16 [100, 256], replicated
- w_two: bfloat16 [256, 47], replicated
- grad_out: float32 [8192, 47], P('rows')
Outputs:
- output 1: float32 [100, 256], replicated
- output 2: float32 [256, 47], replicated
All inputs are finite; a program needn't handle non-finite values.
Results may differ from the reference program's by a relative error of at most 0.001.
Values are sent between devices in bfloat16 or wider.
A program may use at most 1 GiB of HBM per device.

```python
import jax
import jax.numpy as jnp

NUM_NODES = 8192
FEAT_IN = 100
HIDDEN = 256
CLASSES = 47
NEIGHBORS = 32


def setup_inputs(seed: int = 0) -> dict:
    key = jax.random.key(seed)
    key_cols, key_feat, key_one, key_two, key_grad = jax.random.split(key, 5)
    node_ids = jnp.arange(NUM_NODES, dtype=jnp.int32)
    targets = jax.random.randint(key_cols, (NUM_NODES, NEIGHBORS), 0, NUM_NODES, dtype=jnp.int32)
    targets = jnp.concatenate([targets, node_ids[:, None]], axis=1)
    sources = jnp.broadcast_to(node_ids[:, None], targets.shape)
    col_deg = jnp.zeros((NUM_NODES,), jnp.float32).at[targets].add(1.0)
    col_scale = (NEIGHBORS + 1.0) ** -0.5 * col_deg ** -0.5
    edge_vals = col_scale[targets]
    adjacency = jnp.zeros((NUM_NODES, NUM_NODES), jnp.float32).at[sources, targets].add(edge_vals).astype(jnp.bfloat16)
    features = jax.random.normal(key_feat, (NUM_NODES, FEAT_IN), jnp.float32).astype(jnp.bfloat16)
    w_one = (jax.random.normal(key_one, (FEAT_IN, HIDDEN), jnp.float32) * FEAT_IN ** -0.5).astype(jnp.bfloat16)
    w_two = (jax.random.normal(key_two, (HIDDEN, CLASSES), jnp.float32) * HIDDEN ** -0.5).astype(jnp.bfloat16)
    grad_raw = jax.random.normal(key_grad, (NUM_NODES, CLASSES), jnp.float32)
    grad_out = grad_raw - jnp.mean(grad_raw, axis=0, keepdims=True)
    return {"adjacency": adjacency, "features": features, "w_one": w_one, "w_two": w_two, "grad_out": grad_out}


def reference(adjacency, features, w_one, w_two, grad_out):
    act_one = jnp.dot(adjacency, features, preferred_element_type=jnp.float32).astype(jnp.bfloat16)
    hidden = jnp.maximum(jnp.dot(act_one, w_one, preferred_element_type=jnp.float32), 0.0).astype(jnp.bfloat16)
    act_two = jnp.dot(adjacency, hidden, preferred_element_type=jnp.float32).astype(jnp.bfloat16)
    grad_b = grad_out.astype(jnp.bfloat16)
    dw_two = jnp.dot(act_two.T, grad_b, preferred_element_type=jnp.float32)
    d_agg = jnp.dot(grad_b, w_two.T, preferred_element_type=jnp.float32).astype(jnp.bfloat16)
    d_hidden = jnp.dot(d_agg.T, adjacency, preferred_element_type=jnp.float32).T
    d_pre = jnp.where(hidden > 0, d_hidden, 0.0).astype(jnp.bfloat16)
    dw_one = jnp.dot(act_one.T, d_pre, preferred_element_type=jnp.float32)
    return (dw_one, dw_two)
```

```python
import jax
import jax.numpy as jnp
from jax import lax
from jax.experimental import pallas as pl
from jax.experimental.pallas import tpu as pltpu
from jax.sharding import PartitionSpec as P

MESH = pl.DeviceIdType.MESH
F32 = jnp.float32
BF16 = jnp.bfloat16
NN = (((1,), (0,)), ((), ()))
NT = (((1,), (1,)), ((), ()))
TN = (((0,), (0,)), ((), ()))

H_NEAR, H_FAR, HT_D2D, X1_Y, X1_NEAR, X1_FAR, X1_FAR2, X1_D2D = 0, 1, 2, 4, 6, 7, 8, 9
DZ_D2D, DZ_X, X2_Y, AR_ONE, AR_TWO, N_REMOTE = 11, 13, 15, 17, 22, 27
A_CHUNKS = 4


def dot(lhs, rhs, dims):
    return lax.dot_general(lhs, rhs, dims, preferred_element_type=F32)


def ds(start, size, align=128):
    return pl.ds(pl.multiple_of(start, align), size)


def gcn_kernel(
    adj, feat, w_one, w_two, grad, dw1_out, dw2t_out,
    a_v, ht, g_v, w1_v, w2_v, gbt, dyt, dzp, dz_in, dz_s, dz_x,
    x1p, x1_in, x1s, x1t, z1t, x2p, x2_in,
    one_p, one_in, one_all, one_tot, two_p, two_in, two_all, two_tot,
    a_sem, l_sem, send_sem, recv_sem,
):
    y = lax.axis_index("rep")
    r = lax.axis_index("rows")
    x, c = r // 2, lax.rem(r, 2)
    diag = x == y
    peer = (y, 2 * x + 1 - c)
    xn = (y, 2 * (1 - x) + c)
    yn = (1 - y, r)
    opp = (1 - y, 2 * (1 - x) + c)
    rows, cols = a_v.shape
    half, quarter = rows // 2, rows // 4

    def rcopy(src, dst, send, recv, dev):
        return pltpu.make_async_remote_copy(
            src_ref=src, dst_ref=dst, send_sem=send_sem.at[send], recv_sem=recv_sem.at[recv],
            device_id=dev, device_id_type=MESH)

    g_load = pltpu.make_async_copy(grad, g_v, l_sem.at[0])
    w1_load = pltpu.make_async_copy(w_one, w1_v, l_sem.at[1])
    w2_load = pltpu.make_async_copy(w_two, w2_v, l_sem.at[2])
    my_cols, peer_cols = c * rows, (1 - c) * rows
    own_block = ds(my_cols, rows)
    h_load = pltpu.make_async_copy(feat, ht.at[:, own_block], l_sem.at[3])
    g_load.start()
    w1_load.start()
    w2_load.start()

    @pl.when(diag)
    def _():
        h_load.start()

    step = rows // A_CHUNKS
    a_loads = []
    for i in range(A_CHUNKS):
        rng = pl.ds(i * step, step)
        a_loads.append(pltpu.make_async_copy(adj.at[rng], a_v.at[rng], a_sem.at[i]))
        a_loads[-1].start()

    barrier = pltpu.get_barrier_semaphore()
    for dev in (peer, xn, yn, opp):
        pl.semaphore_signal(barrier, inc=1, device_id=dev, device_id_type=MESH)
    pl.semaphore_wait(barrier, 4)

    top, bot = pl.ds(0, half), pl.ds(half, half)
    h_near = rcopy(feat.at[:, top], ht.at[:, ds(my_cols, half)], H_NEAR, H_NEAR, xn)
    h_far = rcopy(feat.at[:, bot], ht.at[:, ds(my_cols + half, half)], H_FAR, H_FAR, opp)

    @pl.when(diag)
    def _():
        h_near.start()

    @pl.when(jnp.logical_not(diag))
    def _():
        h_far.start()

    g_load.wait()
    w2_load.wait()
    gbt[...] = g_v[...].astype(BF16)
    dyt[...] = dot(w2_v[...], gbt[...], TN).astype(BF16)
    for load in a_loads:
        load.wait()

    dz_d2d = []
    for i in range(2):
        cs = ds(peer_cols + i * half, half)
        dzp[:, cs] = dot(dyt[...], a_v[:, cs], NN)
        dz_d2d.append(rcopy(dzp.at[:, cs], dz_in.at[:, pl.ds(i * half, half)], DZ_D2D + i, DZ_D2D + i, peer))
        dz_d2d[-1].start()
    for i in range(2):
        cs = ds(my_cols + i * half, half)
        dzp[:, cs] = dot(dyt[...], a_v[:, cs], NN)

    @pl.when(diag)
    def _():
        h_load.wait()

    @pl.when(jnp.logical_not(diag))
    def _():
        h_near.wait_recv()
        h_far.wait_recv()

    ht_d2d = []
    for i in range(2):
        cs = ds(my_cols + i * half, half)
        ht_d2d.append(rcopy(ht.at[:, cs], ht.at[:, cs], HT_D2D + i, HT_D2D + i, peer))
        ht_d2d[-1].start()
    for copy in ht_d2d:
        copy.wait_recv()

    x1_y = []
    for i in range(2):
        rs = ds((1 - y) * half + i * quarter, quarter)
        x1p[:, rs] = dot(ht[...], a_v[rs, :], NT)
        x1_y.append(rcopy(x1p.at[:, rs], x1_in.at[:, pl.ds(i * quarter, quarter)], X1_Y + i, X1_Y + i, yn))
        x1_y[-1].start()

    dz_d2d[0].wait_recv()
    dz_d2d[1].wait_recv()
    other_x = ds((1 - x) * half, half)
    dz_s[...] = dzp[:, ds(my_cols + (1 - x) * half, half)] + dz_in[:, other_x]
    dz_x_copy = rcopy(dz_s, dz_x, DZ_X, DZ_X, xn)

    for i in range(2):
        rs = ds(y * half + i * quarter, quarter)
        x1p[:, rs] = dot(ht[...], a_v[rs, :], NT)
    for i in range(2):
        x1_y[i].wait_recv()
        rs = ds(y * half + i * quarter, quarter)
        qs = pl.ds(i * quarter, quarter)
        x1s[:, qs] = (x1p[:, rs] + x1_in[:, qs]).astype(BF16)

    slot = ds(c * rows + y * half, half)
    x1_near = rcopy(x1s, x1t.at[:, slot], X1_NEAR, X1_NEAR, xn)
    x1_far = rcopy(x1s, x1t.at[:, slot], X1_FAR, X1_FAR, yn)
    x1_far2 = rcopy(x1s, x1t.at[:, slot], X1_FAR2, X1_FAR, opp)

    @pl.when(diag)
    def _():
        x1_near.start()
        x1t[:, slot] = x1s[...]

    @pl.when(jnp.logical_not(diag))
    def _():
        x1_far2.start()
        x1_far.start()

    dz_x_copy.start()
    w1_load.wait()

    @pl.when(jnp.logical_not(diag))
    def _():
        x1_near.wait_recv()

    near_cols = ds(my_cols + y * half, half)
    far_cols = ds(my_cols + (1 - y) * half, half)
    x1_d2d = [rcopy(x1t.at[:, near_cols], x1t.at[:, near_cols], X1_D2D, X1_D2D, peer),
              rcopy(x1t.at[:, far_cols], x1t.at[:, far_cols], X1_D2D + 1, X1_D2D + 1, peer)]
    x1_d2d[0].start()
    z1t[:, near_cols] = jnp.maximum(dot(w1_v[...], x1t[:, near_cols], TN), 0.0).astype(BF16)
    x1_d2d[0].wait_recv()
    peer_near = ds(peer_cols + y * half, half)
    z1t[:, peer_near] = jnp.maximum(dot(w1_v[...], x1t[:, peer_near], TN), 0.0).astype(BF16)
    x1_far.wait_recv()
    x1_d2d[1].start()
    z1t[:, far_cols] = jnp.maximum(dot(w1_v[...], x1t[:, far_cols], TN), 0.0).astype(BF16)
    x1_d2d[1].wait_recv()
    peer_far = ds(peer_cols + (1 - y) * half, half)
    z1t[:, peer_far] = jnp.maximum(dot(w1_v[...], x1t[:, peer_far], TN), 0.0).astype(BF16)

    x2_y = []
    for i in range(2):
        rs = ds((1 - y) * half + i * quarter, quarter)
        x2p[:, rs] = dot(z1t[...], a_v[rs, :], NT)
        x2_y.append(rcopy(x2p.at[:, rs], x2_in.at[:, pl.ds(i * quarter, quarter)], X2_Y + i, X2_Y + i, yn))
        x2_y[-1].start()
    for i in range(2):
        rs = ds(y * half + i * quarter, quarter)
        x2p[:, rs] = dot(z1t[...], a_v[rs, :], NT)

    def ar_first(part, inn, base):
        n = part.shape[0] // 2
        copy = rcopy(part.at[ds((1 - c) * n, n, 8)], inn, base, base, peer)
        copy.start()
        return copy

    def ar_second(part, inn, alls, base, first):
        n = part.shape[0] // 2
        chip = 2 * x + y
        first.wait_recv()
        alls[chip] = part[ds(c * n, n, 8)] + inn[...]
        copies = []
        for i, dev in enumerate((opp, xn, yn)):
            copies.append(rcopy(alls.at[chip], alls.at[chip], base + 1 + i, base + 1 + i, dev))
            copies[-1].start()
        return copies

    def ar_third(alls, tot, base, second):
        n = alls.shape[1]
        for copy in second:
            copy.wait_recv()
        mine = ds(c * n, n, 8)
        tot[mine] = (alls[0] + alls[1]) + (alls[2] + alls[3])
        copy = rcopy(tot.at[mine], tot.at[mine], base + 4, base + 4, peer)
        copy.start()
        return copy

    own_x = ds(x * half, half)
    dz_cols = ds(my_cols + x * half, half)
    dz_x_copy.wait_recv()
    d_hidden = (dzp[:, dz_cols] + dz_in[:, own_x]) + dz_x[...]
    d_pre = jnp.where(z1t[:, dz_cols].astype(F32) > 0.0, d_hidden, 0.0).astype(BF16)
    feat_in = feat.shape[0]
    one_p[pl.ds(0, feat_in)] = dot(x1t[:, dz_cols], d_pre, NT)
    one_p[pl.ds(feat_in, one_p.shape[0] - feat_in)] = jnp.zeros((one_p.shape[0] - feat_in, one_p.shape[1]), F32)
    one_a = ar_first(one_p, one_in, AR_ONE)
    one_b = ar_second(one_p, one_in, one_all, AR_ONE, one_a)

    classes = grad.shape[0]
    total = None
    for i in range(2):
        x2_y[i].wait_recv()
        rs = ds(y * half + i * quarter, quarter)
        act = (x2p[:, rs] + x2_in[:, pl.ds(i * quarter, quarter)]).astype(BF16)
        part = dot(gbt[:, rs], act, NT)
        total = part if total is None else total + part
    two_p[pl.ds(0, classes)] = total
    two_p[pl.ds(classes, two_p.shape[0] - classes)] = jnp.zeros((two_p.shape[0] - classes, two_p.shape[1]), F32)
    two_a = ar_first(two_p, two_in, AR_TWO)
    one_c = ar_third(one_all, one_tot, AR_ONE, one_b)
    two_b = ar_second(two_p, two_in, two_all, AR_TWO, two_a)
    two_c = ar_third(two_all, two_tot, AR_TWO, two_b)
    one_c.wait_recv()
    dw1_out[...] = one_tot[pl.ds(0, feat_in)]
    two_c.wait_recv()
    dw2t_out[...] = two_tot[pl.ds(0, classes)]

    @pl.when(diag)
    def _():
        h_near.wait_send()
        x1_near.wait_send()

    @pl.when(jnp.logical_not(diag))
    def _():
        h_far.wait_send()
        x1_far.wait_send()
        x1_far2.wait_send()

    for copy in [*ht_d2d, *x1_y, *x1_d2d, *dz_d2d, dz_x_copy, *x2_y, one_a, *one_b, one_c, two_a, *two_b, two_c]:
        copy.wait_send()


def solution(mesh):
    def local_step(adj, feat, w_one, w_two, grad):
        rows, cols = adj.shape
        feat_in, hidden = w_one.shape
        classes = w_two.shape[1]
        half = rows // 2
        fpad, cpad = -(-feat_in // 16) * 16, -(-classes // 16) * 16
        vmem = pltpu.VMEM
        dw1, dw2t = pl.pallas_call(
            gcn_kernel,
            out_shape=(jax.ShapeDtypeStruct((feat_in, hidden), F32), jax.ShapeDtypeStruct((classes, hidden), F32)),
            in_specs=[pl.BlockSpec(memory_space=pltpu.HBM)] * 5,
            out_specs=(pl.BlockSpec(memory_space=vmem), pl.BlockSpec(memory_space=vmem)),
            scratch_shapes=[
                vmem((rows, cols), BF16),
                vmem((feat_in, cols), BF16),
                vmem((classes, rows), F32),
                vmem((feat_in, hidden), BF16),
                vmem((classes, hidden), BF16),
                vmem((classes, rows), BF16),
                vmem((hidden, rows), BF16),
                vmem((hidden, cols), F32),
                vmem((hidden, rows), F32),
                vmem((hidden, half), F32),
                vmem((hidden, half), F32),
                vmem((feat_in, rows), F32),
                vmem((feat_in, half), F32),
                vmem((feat_in, half), BF16),
                vmem((feat_in, cols), BF16),
                vmem((hidden, cols), BF16),
                vmem((hidden, rows), F32),
                vmem((hidden, half), F32),
                vmem((fpad, hidden), F32),
                vmem((fpad // 2, hidden), F32),
                vmem((4, fpad // 2, hidden), F32),
                vmem((fpad, hidden), F32),
                vmem((cpad, hidden), F32),
                vmem((cpad // 2, hidden), F32),
                vmem((4, cpad // 2, hidden), F32),
                vmem((cpad, hidden), F32),
                pltpu.SemaphoreType.DMA((A_CHUNKS,)),
                pltpu.SemaphoreType.DMA((4,)),
                pltpu.SemaphoreType.DMA((N_REMOTE,)),
                pltpu.SemaphoreType.DMA((N_REMOTE,)),
            ],
            compiler_params=pltpu.CompilerParams(
                collective_id=0, has_side_effects=True, vmem_limit_bytes=60 * 1024 * 1024),
        )(adj, feat.T, w_one, w_two.T, grad.T)
        return dw1, dw2t.T

    return jax.shard_map(
        local_step, mesh=mesh,
        in_specs=(P("rows", "rep"), P("rows", None), P(), P(), P("rows", None)),
        out_specs=(P(), P()), check_vma=False)
```

```python
import itertools

import jax
import jax.numpy as jnp
from jax import lax
from jax.experimental import pallas as pl
from jax.experimental.pallas import tpu as pltpu
from jax.sharding import PartitionSpec as P

MESH = pl.DeviceIdType.MESH
F32 = jnp.float32
BF16 = jnp.bfloat16
NN = (((1,), (0,)), ((), ()))
NT = (((1,), (1,)), ((), ()))
TN = (((0,), (0,)), ((), ()))
SUBS = 4
N_SEND = 64
H_R, HT_R, X1Y_R, X1G_R, X1D_R, DZD_R, DZX_R, X2Y_R, ONE_R, TWO_R, N_RECV = 0, 4, 8, 12, 20, 28, 30, 34, 38, 42, 47


def dot(lhs, rhs, dims):
    return lax.dot_general(lhs, rhs, dims, preferred_element_type=F32)


def ds(start, size, align=128):
    return pl.ds(pl.multiple_of(start, align), size)


def gcn_kernel(
    adj, feat, w_one, w_two, grad, dw1_out, dw2t_out,
    a_v, ht, hs, g_v, w1_v, w2_v, gbt, dyt, dzp, dz_in, dz_s, dz_x,
    x1p, x1_in, x1s, x1t, z1t, x2p, x2_in,
    one_p, one_in, one_s, one_x, one_sx, one_y, one_tot, two_p, two_in, two_all, two_tot,
    a_sem, l_sem, send_sem, recv_sem,
):
    y = lax.axis_index("rep")
    r = lax.axis_index("rows")
    x, c = r // 2, lax.rem(r, 2)
    diag = x == y
    off = jnp.logical_not(diag)
    peer = (y, 2 * x + 1 - c)
    xn = (y, 2 * (1 - x) + c)
    yn = (1 - y, r)
    opp = (1 - y, 2 * (1 - x) + c)
    user = (x, 2 * (1 - x) + c)
    rows, cols = a_v.shape
    half, quarter = rows // 2, rows // 4
    sub = half // SUBS
    feat_in, classes = feat.shape[0], grad.shape[0]
    my_cols, peer_cols = c * rows, (1 - c) * rows
    send_ids = itertools.count()
    sent, sent_diag, sent_off = [], [], []

    def rcopy(src, dst, recv, dev, group=sent):
        copy = pltpu.make_async_remote_copy(
            src_ref=src, dst_ref=dst, send_sem=send_sem.at[next(send_ids)], recv_sem=recv_sem.at[recv],
            device_id=dev, device_id_type=MESH)
        group.append(copy)
        return copy

    def wait_recv(dst, recv):
        pltpu.make_async_remote_copy(
            src_ref=dst, dst_ref=dst, send_sem=send_sem.at[0], recv_sem=recv_sem.at[recv],
            device_id=peer, device_id_type=MESH).wait_recv()

    hs_load = pltpu.make_async_copy(feat.at[:, ds(jnp.where(diag, 0, half), half)], hs, l_sem.at[4])
    h_load = pltpu.make_async_copy(feat, ht.at[:, ds(my_cols, rows)], l_sem.at[3])
    hs_load.start()

    @pl.when(diag)
    def _():
        h_load.start()

    g_load = pltpu.make_async_copy(grad, g_v, l_sem.at[0])
    w1_load = pltpu.make_async_copy(w_one, w1_v, l_sem.at[1])
    w2_load = pltpu.make_async_copy(w_two, w2_v, l_sem.at[2])
    g_load.start()
    w1_load.start()
    w2_load.start()
    own0, other0 = y * half, (1 - y) * half
    a_rows = [ds(other0, quarter), ds(other0 + quarter, quarter), ds(own0, quarter), ds(own0 + quarter, quarter)]
    a_loads = [pltpu.make_async_copy(adj.at[rs], a_v.at[rs], a_sem.at[i]) for i, rs in enumerate(a_rows)]
    for load in a_loads:
        load.start()

    barrier = pltpu.get_barrier_semaphore()
    for dev in (peer, xn, yn, opp):
        pl.semaphore_signal(barrier, inc=1, device_id=dev, device_id_type=MESH)
    pl.semaphore_wait(barrier, 4)

    hs_load.wait()
    side = jnp.where(diag, 0, 1)
    for i in range(2):
        rcopy(hs.at[:, pl.ds(i * quarter, quarter)],
              ht.at[:, ds(my_cols + side * half + i * quarter, quarter)], H_R + 2 * side + i, user).start()

    def h_piece(k):
        return ht.at[:, ds(my_cols + k * quarter, quarter)]

    h_fwd = [rcopy(h_piece(k), h_piece(k), HT_R + k, peer) for k in range(4)]

    @pl.when(diag)
    def _():
        h_load.wait()
        for k in range(4):
            h_fwd[k].start()

    g_load.wait()
    w2_load.wait()
    gbt[...] = g_v[...].astype(BF16)
    dyt[...] = dot(w2_v[...], gbt[...], TN).astype(BF16)

    @pl.when(off)
    def _():
        for k in (0, 2, 1, 3):
            wait_recv(h_piece(k), H_R + k)
            h_fwd[k].start()

    own_block, peer_block = ds(my_cols, rows), ds(peer_cols, rows)
    for i in range(2):
        a_loads[i].wait()
        x1p[:, a_rows[i]] = dot(ht[:, own_block], a_v[a_rows[i], own_block], NT)
    for k in range(4):
        h_fwd[k].wait_recv()
    x1_y = []
    for i in range(2):
        x1p[:, a_rows[i]] += dot(ht[:, peer_block], a_v[a_rows[i], peer_block], NT)
        for j in range(2 * i, 2 * i + 2):
            x1_y.append(rcopy(x1p.at[:, ds(other0 + j * sub, sub)], x1_in.at[:, pl.ds(j * sub, sub)], X1Y_R + j, yn))
            x1_y[-1].start()
    for i in range(2, 4):
        a_loads[i].wait()
        x1p[:, a_rows[i]] = dot(ht[...], a_v[a_rows[i], :], NT)

    dz_d2d = []

    def backward(start):
        cs = ds(start, half)
        dzp[:, cs] = dot(dyt[...], a_v[:, cs], NN)

    def mine(ref, h, i):
        return ref.at[:, ds(my_cols + h * half + i * sub, sub)]

    x1_fwd = {(h, i): rcopy(mine(x1t, hv, i), mine(x1t, hv, i), X1D_R + 4 * h + i, peer)
              for h, hv in ((0, x), (1, 1 - x)) for i in range(SUBS)}
    x1_user, x1_col = [], []

    def sum_x1(i):
        x1_y[i].wait_recv()
        cs = pl.ds(i * sub, sub)
        act = (x1p[:, ds(own0 + i * sub, sub)] + x1_in[:, cs]).astype(BF16)
        x1s[:, cs] = act
        x1_user.append(rcopy(x1s.at[:, cs], mine(x1t, y, i), X1G_R + 4 * y + i, user))
        x1_col.append(rcopy(x1s.at[:, cs], mine(x1t, y, i), X1G_R + 4 * y + i, yn, sent_off))
        x1_user[-1].start()

        @pl.when(diag)
        def _():
            mine(x1t, y, i)[...] = act
            x1_fwd[0, i].start()

        @pl.when(off)
        def _():
            x1_col[i].start()

    for i in range(2):
        backward(peer_cols + i * half)
        dz_d2d.append(rcopy(dzp.at[:, ds(peer_cols + i * half, half)], dz_in.at[:, pl.ds(i * half, half)], DZD_R + i, peer))
        dz_d2d[-1].start()
    sum_x1(0)
    backward(my_cols)
    sum_x1(1)
    backward(my_cols + half)
    sum_x1(2)
    for copy in dz_d2d:
        copy.wait_recv()
    dz_s[...] = dzp[:, ds(my_cols + (1 - x) * half, half)] + dz_in[:, ds((1 - x) * half, half)]
    sum_x1(3)
    dz_x_copies = []
    for i in range(SUBS):
        cs = pl.ds(i * sub, sub)
        dz_x_copies.append(rcopy(dz_s.at[:, cs], dz_x.at[:, cs], DZX_R + i, xn))
        dz_x_copies[-1].start()

    w1_load.wait()

    def hidden(start, size):
        cs = ds(start, size)
        z1t[:, cs] = jnp.maximum(dot(w1_v[...], x1t[:, cs], TN), 0.0).astype(BF16)

    for i in range(SUBS):
        @pl.when(off)
        def _():
            wait_recv(mine(x1t, x, i), X1G_R + 4 * x + i)
            x1_fwd[0, i].start()
    hidden(my_cols + x * half, half)
    for i in range(SUBS):
        x1_fwd[0, i].wait_recv()
    hidden(peer_cols + x * half, half)
    first_own, first_peer = ds(my_cols + x * half, half), ds(peer_cols + x * half, half)
    for i in range(SUBS):
        rs = a_rows[i]
        x2p[:, rs] = dot(z1t[:, first_own], a_v[rs, first_own], NT) + dot(z1t[:, first_peer], a_v[rs, first_peer], NT)
        wait_recv(mine(x1t, 1 - x, i), X1G_R + 4 * (1 - x) + i)
        x1_fwd[1, i].start()
        hidden(my_cols + (1 - x) * half + i * sub, sub)
    for i in range(SUBS):
        x1_fwd[1, i].wait_recv()
        hidden(peer_cols + (1 - x) * half + i * sub, sub)
    last_own, last_peer = ds(my_cols + (1 - x) * half, half), ds(peer_cols + (1 - x) * half, half)
    x2_y = []
    for i in range(SUBS):
        rs = a_rows[i]
        x2p[:, rs] += dot(z1t[:, last_own], a_v[rs, last_own], NT) + dot(z1t[:, last_peer], a_v[rs, last_peer], NT)
        if i < 2:
            for j in range(2 * i, 2 * i + 2):
                x2_y.append(rcopy(x2p.at[:, ds(other0 + j * sub, sub)], x2_in.at[:, pl.ds(j * sub, sub)], X2Y_R + j, yn))
                x2_y[-1].start()

    dw1 = None
    for i in range(SUBS):
        dz_x_copies[i].wait_recv()
        cs = ds(my_cols + x * half + i * sub, sub)
        d_hidden = (dzp[:, cs] + dz_in[:, ds(x * half + i * sub, sub)]) + dz_x[:, pl.ds(i * sub, sub)]
        d_pre = jnp.where(z1t[:, cs].astype(F32) > 0.0, d_hidden, 0.0).astype(BF16)
        part = dot(x1t[:, cs], d_pre, NT)
        dw1 = part if dw1 is None else dw1 + part
    one_p[pl.ds(0, feat_in)] = dw1
    one_p[pl.ds(feat_in, one_p.shape[0] - feat_in)] = jnp.zeros((one_p.shape[0] - feat_in, one_p.shape[1]), F32)

    n_one = one_p.shape[0] // 2
    one_a = rcopy(one_p.at[ds((1 - c) * n_one, n_one, 8)], one_in, ONE_R, peer)
    one_a.start()
    one_a.wait_recv()
    one_s[...] = one_p[ds(c * n_one, n_one, 8)] + one_in[...]
    one_b = rcopy(one_s, one_x, ONE_R + 1, xn)
    one_b.start()
    one_b.wait_recv()
    one_sx[...] = one_s[...] + one_x[...]
    one_c = rcopy(one_sx, one_y, ONE_R + 2, yn)
    one_c.start()

    dw2 = None
    for i in range(SUBS):
        x2_y[i].wait_recv()
        rs = ds(own0 + i * sub, sub)
        act = (x2p[:, rs] + x2_in[:, pl.ds(i * sub, sub)]).astype(BF16)
        part = dot(gbt[:, rs], act, NT)
        dw2 = part if dw2 is None else dw2 + part
    two_p[pl.ds(0, classes)] = dw2
    two_p[pl.ds(classes, two_p.shape[0] - classes)] = jnp.zeros((two_p.shape[0] - classes, two_p.shape[1]), F32)

    n_two = two_p.shape[0] // 2
    chip = 2 * x + y
    two_a = rcopy(two_p.at[ds((1 - c) * n_two, n_two, 8)], two_in, TWO_R, peer)
    two_a.start()
    one_c.wait_recv()
    one_mine = ds(c * n_one, n_one, 8)
    one_tot[one_mine] = one_sx[...] + one_y[...]
    one_d = rcopy(one_tot.at[one_mine], one_tot.at[one_mine], ONE_R + 3, peer)
    one_d.start()
    two_a.wait_recv()
    two_all[chip] = two_p[ds(c * n_two, n_two, 8)] + two_in[...]
    two_b = [rcopy(two_all.at[chip], two_all.at[chip], TWO_R + 1 + i, dev) for i, dev in enumerate((opp, xn, yn))]
    for copy in two_b:
        copy.start()
    one_d.wait_recv()
    dw1_out[...] = one_tot[pl.ds(0, feat_in)]
    for copy in two_b:
        copy.wait_recv()
    two_mine = ds(c * n_two, n_two, 8)
    two_tot[two_mine] = (two_all[0] + two_all[1]) + (two_all[2] + two_all[3])
    two_c = rcopy(two_tot.at[two_mine], two_tot.at[two_mine], TWO_R + 4, peer)
    two_c.start()
    two_c.wait_recv()
    dw2t_out[...] = two_tot[pl.ds(0, classes)]

    for copy in sent:
        copy.wait_send()

    @pl.when(off)
    def _():
        for copy in sent_off:
            copy.wait_send()


def solution(mesh):
    def local_step(adj, feat, w_one, w_two, grad):
        rows, cols = adj.shape
        feat_in, hidden = w_one.shape
        classes = w_two.shape[1]
        half = rows // 2
        fpad, cpad = -(-feat_in // 16) * 16, -(-classes // 16) * 16
        vmem = pltpu.VMEM
        one_half = vmem((fpad // 2, hidden), F32)
        dw1, dw2t = pl.pallas_call(
            gcn_kernel,
            out_shape=(jax.ShapeDtypeStruct((feat_in, hidden), F32), jax.ShapeDtypeStruct((classes, hidden), F32)),
            in_specs=[pl.BlockSpec(memory_space=pltpu.HBM)] * 5,
            out_specs=(pl.BlockSpec(memory_space=vmem), pl.BlockSpec(memory_space=vmem)),
            scratch_shapes=[
                vmem((rows, cols), BF16),
                vmem((feat_in, cols), BF16),
                vmem((feat_in, half), BF16),
                vmem((classes, rows), F32),
                vmem((feat_in, hidden), BF16),
                vmem((classes, hidden), BF16),
                vmem((classes, rows), BF16),
                vmem((hidden, rows), BF16),
                vmem((hidden, cols), F32),
                vmem((hidden, rows), F32),
                vmem((hidden, half), F32),
                vmem((hidden, half), F32),
                vmem((feat_in, rows), F32),
                vmem((feat_in, half), F32),
                vmem((feat_in, half), BF16),
                vmem((feat_in, cols), BF16),
                vmem((hidden, cols), BF16),
                vmem((hidden, rows), F32),
                vmem((hidden, half), F32),
                vmem((fpad, hidden), F32),
                *[one_half] * 5,
                vmem((fpad, hidden), F32),
                vmem((cpad, hidden), F32),
                vmem((cpad // 2, hidden), F32),
                vmem((4, cpad // 2, hidden), F32),
                vmem((cpad, hidden), F32),
                pltpu.SemaphoreType.DMA((4,)),
                pltpu.SemaphoreType.DMA((5,)),
                pltpu.SemaphoreType.DMA((N_SEND,)),
                pltpu.SemaphoreType.DMA((N_RECV,)),
            ],
            compiler_params=pltpu.CompilerParams(
                collective_id=0, has_side_effects=True, vmem_limit_bytes=60 * 1024 * 1024),
        )(adj, feat.T, w_one, w_two.T, grad.T)
        return dw1, dw2t.T

    return jax.shard_map(
        local_step, mesh=mesh,
        in_specs=(P("rows", "rep"), P("rows", None), P(), P(), P("rows", None)),
        out_specs=(P(), P()), check_vma=False)
```

```python
import itertools

import jax
import jax.numpy as jnp
from jax import lax
from jax.experimental import pallas as pl
from jax.experimental.pallas import tpu as pltpu
from jax.sharding import PartitionSpec as P

MESH = pl.DeviceIdType.MESH
F32 = jnp.float32
BF16 = jnp.bfloat16
NN = (((1,), (0,)), ((), ()))
NT = (((1,), (1,)), ((), ()))
TN = (((0,), (0,)), ((), ()))
SUBS = 4
N_SEND = 64
H_R, HT_R, X1Y_R, X1G_R, X1D_R, DZD_R, DZX_R, X2Y_R, ONE_R, TWO_R, N_RECV = 0, 4, 8, 12, 20, 28, 30, 34, 38, 42, 47


def dot(lhs, rhs, dims):
    return lax.dot_general(lhs, rhs, dims, preferred_element_type=F32)


def ds(start, size, align=128):
    return pl.ds(pl.multiple_of(start, align), size)


def gcn_kernel(
    adj, feat, w_one, w_two, grad, dw1_out, dw2t_out,
    a_v, ht, hs, g_v, w1_v, w2_v, gbt, dyt, dzp, dz_in, dz_s, dz_x,
    x1p, x1_in, x1s, x1t, z1t, x2p, x2_in,
    one_p, one_in, one_s, one_x, one_sx, one_y, one_tot, two_p, two_in, two_all, two_tot,
    a_sem, l_sem, send_sem, recv_sem,
):
    y = lax.axis_index("rep")
    r = lax.axis_index("rows")
    x, c = r // 2, lax.rem(r, 2)
    diag = x == y
    off = jnp.logical_not(diag)
    peer = (y, 2 * x + 1 - c)
    xn = (y, 2 * (1 - x) + c)
    yn = (1 - y, r)
    opp = (1 - y, 2 * (1 - x) + c)
    user = (x, 2 * (1 - x) + c)
    rows, cols = a_v.shape
    half, quarter = rows // 2, rows // 4
    sub = half // SUBS
    feat_in, classes = feat.shape[0], grad.shape[0]
    my_cols, peer_cols = c * rows, (1 - c) * rows
    send_ids = itertools.count()
    sent, sent_diag, sent_off = [], [], []

    def rcopy(src, dst, recv, dev, group=sent):
        copy = pltpu.make_async_remote_copy(
            src_ref=src, dst_ref=dst, send_sem=send_sem.at[next(send_ids)], recv_sem=recv_sem.at[recv],
            device_id=dev, device_id_type=MESH)
        group.append(copy)
        return copy

    def wait_recv(dst, recv):
        pltpu.make_async_remote_copy(
            src_ref=dst, dst_ref=dst, send_sem=send_sem.at[0], recv_sem=recv_sem.at[recv],
            device_id=peer, device_id_type=MESH).wait_recv()

    side = jnp.where(diag, 0, 1)
    hs_loads = [pltpu.make_async_copy(feat.at[:, ds((2 * w + side) * quarter, quarter)],
                                      hs.at[:, pl.ds(w * quarter, quarter)], l_sem.at[4 + w]) for w in range(2)]
    h_load = pltpu.make_async_copy(feat, ht.at[:, ds(my_cols, rows)], l_sem.at[3])
    for load in hs_loads:
        load.start()

    @pl.when(diag)
    def _():
        h_load.start()

    g_load = pltpu.make_async_copy(grad, g_v, l_sem.at[0])
    w1_load = pltpu.make_async_copy(w_one, w1_v, l_sem.at[1])
    w2_load = pltpu.make_async_copy(w_two, w2_v, l_sem.at[2])
    own0, other0 = y * half, (1 - y) * half
    a_rows = [ds(other0, quarter), ds(other0 + quarter, quarter), ds(own0, quarter), ds(own0 + quarter, quarter)]
    a_loads = []
    for i, start in enumerate((other0, other0 + quarter, own0, own0 + quarter)):
        for j in range(2):
            rs = ds(start + j * sub, sub)
            a_loads.append(pltpu.make_async_copy(adj.at[rs], a_v.at[rs], a_sem.at[2 * i + j]))
    for load in a_loads[:4]:
        load.start()

    def wait_a(i):
        a_loads[2 * i].wait()
        a_loads[2 * i + 1].wait()

    barrier = pltpu.get_barrier_semaphore()
    for dev in (peer, xn, yn, opp):
        pl.semaphore_signal(barrier, inc=1, device_id=dev, device_id_type=MESH)
    pl.semaphore_wait(barrier, 4)

    def h_piece(k):
        return ht.at[:, ds(my_cols + k * quarter, quarter)]

    for w in range(2):
        hs_loads[w].wait()
        rcopy(hs.at[:, pl.ds(w * quarter, quarter)], h_piece(2 * w + side), H_R + 2 * w + side, user).start()

    for load in a_loads[4:]:
        load.start()
    for load in (g_load, w1_load, w2_load):
        load.start()
    h_fwd = [rcopy(h_piece(k), h_piece(k), HT_R + k, peer) for k in range(4)]

    @pl.when(diag)
    def _():
        h_load.wait()
        for k in range(4):
            h_fwd[k].start()

    x1_y = []

    def add_x1(i, cs, first=False):
        part = dot(ht[:, cs], a_v[a_rows[i], cs], NT)
        x1p[:, a_rows[i]] = part if first else x1p[:, a_rows[i]] + part

    for j in range(SUBS):
        x1_y.append(rcopy(x1p.at[:, ds(other0 + j * sub, sub)], x1_in.at[:, pl.ds(j * sub, sub)], X1Y_R + j, yn))

    def send_x1(i, role):
        @pl.when(role)
        def _():
            x1_y[2 * i].start()
            x1_y[2 * i + 1].start()

    def forward_h(w):
        @pl.when(off)
        def _():
            for k in (2 * w, 2 * w + 1):
                wait_recv(h_piece(k), H_R + k)
                h_fwd[k].start()

    waves = [(ds(my_cols + w * half, half), ds(peer_cols + w * half, half)) for w in range(2)]
    forward_h(0)
    for i in range(2):
        wait_a(i)
        add_x1(i, waves[0][0], True)
    for k in range(2):
        h_fwd[k].wait_recv()
    for i in range(2):
        add_x1(i, waves[0][1])
    forward_h(1)
    add_x1(0, waves[1][0])
    for k in range(2, 4):
        h_fwd[k].wait_recv()
    add_x1(0, waves[1][1])
    send_x1(0, off)
    add_x1(1, waves[1][0])
    add_x1(1, waves[1][1])
    send_x1(0, diag)
    send_x1(1, diag)
    send_x1(1, off)
    for i in range(2, 4):
        wait_a(i)
        x1p[:, a_rows[i]] = dot(ht[...], a_v[a_rows[i], :], NT)

    dz_d2d = []

    def backward(start):
        cs = ds(start, half)
        dzp[:, cs] = dot(dyt[...], a_v[:, cs], NN)

    def mine(ref, h, i):
        return ref.at[:, ds(my_cols + h * half + i * sub, sub)]

    x1_fwd = {(h, i): rcopy(mine(x1t, hv, i), mine(x1t, hv, i), X1D_R + 4 * h + i, peer)
              for h, hv in ((0, y), (1, 1 - y)) for i in range(SUBS)}
    x1_user, x1_col = [], []

    for i in range(SUBS):
        piece = x1s.at[:, pl.ds(i * sub, sub)]
        x1_user.append(rcopy(piece, mine(x1t, y, i), X1G_R + 4 * y + i, user))
        x1_col.append(rcopy(piece, mine(x1t, y, i), X1G_R + 4 * y + i, yn, sent_off))

    def sum_x1(i):
        x1_y[i].wait_recv()
        cs = pl.ds(i * sub, sub)
        act = (x1p[:, ds(own0 + i * sub, sub)] + x1_in[:, cs]).astype(BF16)
        x1s[:, cs] = act
        x1_user[i].start()

        @pl.when(diag)
        def _():
            mine(x1t, y, i)[...] = act
            x1_fwd[0, i].start()

        @pl.when(off)
        def _():
            x1_col[i].start()

    g_load.wait()
    w2_load.wait()
    gbt[...] = g_v[...].astype(BF16)
    dyt[...] = dot(w2_v[...], gbt[...], TN).astype(BF16)

    for i in range(2):
        backward(peer_cols + i * half)
        dz_d2d.append(rcopy(dzp.at[:, ds(peer_cols + i * half, half)], dz_in.at[:, pl.ds(i * half, half)], DZD_R + i, peer))
        dz_d2d[-1].start()
        sum_x1(i)
    backward(my_cols)
    sum_x1(2)
    backward(my_cols + half)
    for copy in dz_d2d:
        copy.wait_recv()
    dz_s[...] = dzp[:, ds(my_cols + (1 - x) * half, half)] + dz_in[:, ds((1 - x) * half, half)]
    sum_x1(3)
    dz_x_copies = []
    for i in range(SUBS):
        cs = pl.ds(i * sub, sub)
        dz_x_copies.append(rcopy(dz_s.at[:, cs], dz_x.at[:, cs], DZX_R + i, xn))

    def send_dz(role):
        @pl.when(role)
        def _():
            for copy in dz_x_copies:
                copy.start()

    send_dz(off)
    w1_load.wait()

    def hidden(start, size):
        cs = ds(start, size)
        z1t[:, cs] = jnp.maximum(dot(w1_v[...], x1t[:, cs], TN), 0.0).astype(BF16)

    halves = (y * half, (1 - y) * half)

    def own_piece(i):
        @pl.when(off)
        def _():
            wait_recv(mine(x1t, y, i), X1G_R + 4 * y + i)
            x1_fwd[0, i].start()

        wait_recv(mine(x1t, 1 - y, i), X1G_R + 4 * (1 - y) + i)
        x1_fwd[1, i].start()
        for h in halves:
            hidden(my_cols + h + i * sub, sub)

    def peer_piece(i):
        x1_fwd[0, i].wait_recv()
        x1_fwd[1, i].wait_recv()
        for h in halves:
            hidden(peer_cols + h + i * sub, sub)

    def part_x2(rs, block, group):
        total = None
        for h in halves:
            cs = ds(block + h + group * quarter, quarter)
            part = dot(z1t[:, cs], a_v[rs, cs], NT)
            total = part if total is None else total + part
        return total

    own_piece(0)
    send_dz(diag)
    own_piece(1)
    peer_piece(0)
    peer_piece(1)
    x2p[:, a_rows[0]] = part_x2(a_rows[0], my_cols, 0) + part_x2(a_rows[0], peer_cols, 0)
    own_piece(2)
    x2p[:, a_rows[1]] = part_x2(a_rows[1], my_cols, 0) + part_x2(a_rows[1], peer_cols, 0)
    own_piece(3)
    peer_piece(2)
    x2p[:, a_rows[0]] += part_x2(a_rows[0], my_cols, 1)
    peer_piece(3)
    x2_y = []
    for j in range(SUBS):
        rs = ds(other0 + j * sub, sub)
        more = part_x2(rs, peer_cols, 1)
        if j >= 2:
            more = more + part_x2(rs, my_cols, 1)
        x2p[:, rs] += more
        x2_y.append(rcopy(x2p.at[:, rs], x2_in.at[:, pl.ds(j * sub, sub)], X2Y_R + j, yn))
        x2_y[-1].start()
    for rs in a_rows[2:]:
        x2p[:, rs] = dot(z1t[...], a_v[rs, :], NT)

    dw1 = None
    for i in range(SUBS):
        dz_x_copies[i].wait_recv()
        cs = ds(my_cols + x * half + i * sub, sub)
        d_hidden = (dzp[:, cs] + dz_in[:, ds(x * half + i * sub, sub)]) + dz_x[:, pl.ds(i * sub, sub)]
        d_pre = jnp.where(z1t[:, cs].astype(F32) > 0.0, d_hidden, 0.0).astype(BF16)
        part = dot(x1t[:, cs], d_pre, NT)
        dw1 = part if dw1 is None else dw1 + part
    one_p[pl.ds(0, feat_in)] = dw1
    one_p[pl.ds(feat_in, one_p.shape[0] - feat_in)] = jnp.zeros((one_p.shape[0] - feat_in, one_p.shape[1]), F32)

    n_one = one_p.shape[0] // 2
    one_a = rcopy(one_p.at[ds((1 - c) * n_one, n_one, 8)], one_in, ONE_R, peer)
    one_a.start()
    one_a.wait_recv()
    one_s[...] = one_p[ds(c * n_one, n_one, 8)] + one_in[...]
    one_b = rcopy(one_s, one_x, ONE_R + 1, xn)
    one_b.start()
    one_b.wait_recv()
    one_sx[...] = one_s[...] + one_x[...]
    one_c = rcopy(one_sx, one_y, ONE_R + 2, yn)
    one_c.start()

    dw2 = None
    for i in range(SUBS):
        x2_y[i].wait_recv()
        rs = ds(own0 + i * sub, sub)
        act = (x2p[:, rs] + x2_in[:, pl.ds(i * sub, sub)]).astype(BF16)
        part = dot(gbt[:, rs], act, NT)
        dw2 = part if dw2 is None else dw2 + part
    two_p[pl.ds(0, classes)] = dw2
    two_p[pl.ds(classes, two_p.shape[0] - classes)] = jnp.zeros((two_p.shape[0] - classes, two_p.shape[1]), F32)

    n_two = two_p.shape[0] // 2
    chip = 2 * x + y
    two_a = rcopy(two_p.at[ds((1 - c) * n_two, n_two, 8)], two_in, TWO_R, peer)
    two_a.start()
    one_c.wait_recv()
    one_mine = ds(c * n_one, n_one, 8)
    one_tot[one_mine] = one_sx[...] + one_y[...]
    one_d = rcopy(one_tot.at[one_mine], one_tot.at[one_mine], ONE_R + 3, peer)
    one_d.start()
    two_a.wait_recv()
    two_all[chip] = two_p[ds(c * n_two, n_two, 8)] + two_in[...]
    two_b = [rcopy(two_all.at[chip], two_all.at[chip], TWO_R + 1 + i, dev) for i, dev in enumerate((opp, xn, yn))]
    for copy in two_b:
        copy.start()
    one_d.wait_recv()
    dw1_store = pltpu.make_async_copy(one_tot, dw1_out, l_sem.at[6])
    dw1_store.start()
    for copy in two_b:
        copy.wait_recv()
    two_mine = ds(c * n_two, n_two, 8)
    two_tot[two_mine] = (two_all[0] + two_all[1]) + (two_all[2] + two_all[3])
    two_c = rcopy(two_tot.at[two_mine], two_tot.at[two_mine], TWO_R + 4, peer)
    two_c.start()
    two_c.wait_recv()
    dw2_store = pltpu.make_async_copy(two_tot, dw2t_out, l_sem.at[7])
    dw2_store.start()

    for copy in sent:
        copy.wait_send()

    @pl.when(off)
    def _():
        for copy in sent_off:
            copy.wait_send()
    dw1_store.wait()
    dw2_store.wait()


def solution(mesh):
    def local_step(adj, feat, w_one, w_two, grad):
        rows, cols = adj.shape
        feat_in, hidden = w_one.shape
        classes = w_two.shape[1]
        half = rows // 2
        fpad, cpad = -(-feat_in // 16) * 16, -(-classes // 16) * 16
        vmem = pltpu.VMEM
        one_half = vmem((fpad // 2, hidden), F32)
        dw1, dw2t = pl.pallas_call(
            gcn_kernel,
            out_shape=(jax.ShapeDtypeStruct((fpad, hidden), F32), jax.ShapeDtypeStruct((cpad, hidden), F32)),
            in_specs=[pl.BlockSpec(memory_space=pltpu.HBM)] * 5,
            out_specs=(pl.BlockSpec(memory_space=pltpu.HBM), pl.BlockSpec(memory_space=pltpu.HBM)),
            scratch_shapes=[
                vmem((rows, cols), BF16),
                vmem((feat_in, cols), BF16),
                vmem((feat_in, half), BF16),
                vmem((classes, rows), F32),
                vmem((feat_in, hidden), BF16),
                vmem((classes, hidden), BF16),
                vmem((classes, rows), BF16),
                vmem((hidden, rows), BF16),
                vmem((hidden, cols), F32),
                vmem((hidden, rows), F32),
                vmem((hidden, half), F32),
                vmem((hidden, half), F32),
                vmem((feat_in, rows), F32),
                vmem((feat_in, half), F32),
                vmem((feat_in, half), BF16),
                vmem((feat_in, cols), BF16),
                vmem((hidden, cols), BF16),
                vmem((hidden, rows), F32),
                vmem((hidden, half), F32),
                vmem((fpad, hidden), F32),
                *[one_half] * 5,
                vmem((fpad, hidden), F32),
                vmem((cpad, hidden), F32),
                vmem((cpad // 2, hidden), F32),
                vmem((4, cpad // 2, hidden), F32),
                vmem((cpad, hidden), F32),
                pltpu.SemaphoreType.DMA((8,)),
                pltpu.SemaphoreType.DMA((8,)),
                pltpu.SemaphoreType.DMA((N_SEND,)),
                pltpu.SemaphoreType.DMA((N_RECV,)),
            ],
            compiler_params=pltpu.CompilerParams(
                collective_id=0, has_side_effects=True, vmem_limit_bytes=60 * 1024 * 1024),
        )(adj, feat.T, w_one, w_two.T, grad.T)
        return dw1[:feat_in], dw2t[:classes].T

    return jax.shard_map(
        local_step, mesh=mesh,
        in_specs=(P("rows", "rep"), P("rows", None), P(), P(), P("rows", None)),
        out_specs=(P(), P()), check_vma=False)
```

```python
import jax
import jax.numpy as jnp
from jax import lax
from jax.experimental import pallas as pl
from jax.experimental.pallas import tpu as pltpu
from jax.sharding import PartitionSpec as P

MESH = pl.DeviceIdType.MESH
F32 = jnp.float32
BF16 = jnp.bfloat16
NN = (((1,), (0,)), ((), ()))
NT = (((1,), (1,)), ((), ()))
TN = (((0,), (0,)), ((), ()))
SUBS = 4
H_S, HT_S, X1Y_S, X1U_S, X1C_S, X1D_S, DZD_S, DZX_S, X2Y_S, ONE_S, TWO_S, N_SEND = 0, 1, 2, 3, 4, 5, 6, 7, 8, 9, 13, 16
H_R, HT_R, X1Y_R, X1G_R, X1D_R, DZD_R, DZX_R, X2Y_R, ONE_R, TWO_R, N_RECV = 0, 2, 4, 8, 16, 20, 21, 23, 25, 29, 32


def dot(lhs, rhs, dims):
    return lax.dot_general(lhs, rhs, dims, preferred_element_type=F32)


def ds(start, size, align=128):
    return pl.ds(pl.multiple_of(start, align), size)


def gcn_kernel(
    adj, feat, w_one, w_two, grad, dw1_out, dw2t_out,
    a_v, ht, hs, g_v, w1_v, w2_v, gbt, dyt, dzp, dz_in, dz_s, dz_x,
    x1p, x1_in, x1s, x1t, z1t, x2p, x2_in,
    one_p, one_in, one_s, one_x, one_sx, one_y, one_tot, two_p, two_in, two_all, two_tot,
    a_sem, l_sem, send_sem, recv_sem,
):
    y = lax.axis_index("rep")
    r = lax.axis_index("rows")
    x, c = r // 2, lax.rem(r, 2)
    diag = x == y
    off = jnp.logical_not(diag)
    peer = (y, 2 * x + 1 - c)
    xn = (y, 2 * (1 - x) + c)
    yn = (1 - y, r)
    opp = (1 - y, 2 * (1 - x) + c)
    user = (x, 2 * (1 - x) + c)
    rows, cols = a_v.shape
    half, quarter = rows // 2, rows // 4
    sub = half // SUBS
    feat_in, classes = feat.shape[0], grad.shape[0]
    my_cols, peer_cols = c * rows, (1 - c) * rows

    def rcopy(src, dst, send, recv, dev):
        return pltpu.make_async_remote_copy(
            src_ref=src, dst_ref=dst, send_sem=send_sem.at[send], recv_sem=recv_sem.at[recv],
            device_id=dev, device_id_type=MESH)

    def wait_recv(dst, recv):
        rcopy(dst, dst, 0, recv, peer).wait_recv()

    def wait_send(src, send):
        rcopy(src, src, send, 0, peer).wait_send()

    side = jnp.where(diag, 0, 1)
    hs_loads = [pltpu.make_async_copy(feat.at[:, ds((2 * w + side) * quarter, quarter)],
                                      hs.at[:, pl.ds(w * quarter, quarter)], l_sem.at[4 + w]) for w in range(2)]
    h_load = pltpu.make_async_copy(feat, ht.at[:, ds(my_cols, rows)], l_sem.at[3])
    for load in hs_loads:
        load.start()

    @pl.when(diag)
    def _():
        h_load.start()

    g_load = pltpu.make_async_copy(grad, g_v, l_sem.at[0])
    w1_load = pltpu.make_async_copy(w_one, w1_v, l_sem.at[1])
    w2_load = pltpu.make_async_copy(w_two, w2_v, l_sem.at[2])
    own0, other0 = y * half, (1 - y) * half
    a_rows = [ds(other0, quarter), ds(other0 + quarter, quarter), ds(own0, quarter), ds(own0 + quarter, quarter)]
    a_loads = []
    for i, start in enumerate((other0, other0 + quarter, own0, own0 + quarter)):
        for j in range(2):
            rs = ds(start + j * sub, sub)
            a_loads.append(pltpu.make_async_copy(adj.at[rs], a_v.at[rs], a_sem.at[i]))
    for load in a_loads[:4]:
        load.start()

    def wait_a(i):
        pltpu.make_async_copy(adj.at[a_rows[i]], a_v.at[a_rows[i]], a_sem.at[i]).wait()

    barrier = pltpu.get_barrier_semaphore()
    for dev in (peer, xn, yn, opp):
        pl.semaphore_signal(barrier, inc=1, device_id=dev, device_id_type=MESH)
    pl.semaphore_wait(barrier, 4)

    def h_piece(k):
        return ht.at[:, ds(my_cols + k * quarter, quarter)]

    for w in range(2):
        hs_loads[w].wait()
        rcopy(hs.at[:, pl.ds(w * quarter, quarter)], h_piece(2 * w + side), H_S, H_R + w, user).start()

    for load in a_loads[4:]:
        load.start()
    for load in (g_load, w1_load, w2_load):
        load.start()
    def h_wave(w, start):
        return ht.at[:, ds(start + w * half, half)]

    h_fwd = [rcopy(h_wave(w, my_cols), h_wave(w, my_cols), HT_S, HT_R + w, peer) for w in range(2)]

    @pl.when(diag)
    def _():
        h_load.wait()
        for w in range(2):
            h_fwd[w].start()

    x1_y = []

    def add_x1(i, cs, first=False):
        part = dot(ht[:, cs], a_v[a_rows[i], cs], NT)
        x1p[:, a_rows[i]] = part if first else x1p[:, a_rows[i]] + part

    for j in range(SUBS):
        x1_y.append(rcopy(x1p.at[:, ds(other0 + j * sub, sub)], x1_in.at[:, pl.ds(j * sub, sub)], X1Y_S, X1Y_R + j, yn))

    def send_x1(i, role):
        @pl.when(role)
        def _():
            x1_y[2 * i].start()
            x1_y[2 * i + 1].start()

    def forward_h(w):
        @pl.when(off)
        def _():
            wait_recv(h_wave(w, my_cols), H_R + w)
            h_fwd[w].start()

    waves = [(ds(my_cols + w * half, half), ds(peer_cols + w * half, half)) for w in range(2)]
    forward_h(0)
    for i in range(2):
        wait_a(i)
        add_x1(i, waves[0][0], True)
    h_fwd[0].wait_recv()
    for i in range(2):
        add_x1(i, waves[0][1])
    forward_h(1)
    add_x1(0, waves[1][0])
    h_fwd[1].wait_recv()
    add_x1(0, waves[1][1])
    send_x1(0, off)
    add_x1(1, waves[1][0])
    add_x1(1, waves[1][1])
    send_x1(0, diag)
    send_x1(1, diag)
    send_x1(1, off)
    for i in range(2, 4):
        wait_a(i)
        x1p[:, a_rows[i]] = dot(ht[...], a_v[a_rows[i], :], NT)

    dz_d2d = []

    def backward(start):
        cs = ds(start, half)
        dzp[:, cs] = dot(dyt[...], a_v[:, cs], NN)

    def mine(ref, h, i):
        return ref.at[:, ds(my_cols + h * half + i * sub, sub)]

    x1_fwd = {(h, i): rcopy(mine(x1t, hv, i), mine(x1t, hv, i), X1D_S, X1D_R + i, peer)
              for h, hv in ((0, y), (1, 1 - y)) for i in range(SUBS)}
    x1_user, x1_col = [], []

    for i in range(SUBS):
        piece = x1s.at[:, pl.ds(i * sub, sub)]
        x1_user.append(rcopy(piece, mine(x1t, y, i), X1U_S, X1G_R + 4 * y + i, user))
        x1_col.append(rcopy(piece, mine(x1t, y, i), X1C_S, X1G_R + 4 * y + i, yn))

    def sum_x1(i):
        x1_y[i].wait_recv()
        cs = pl.ds(i * sub, sub)
        act = (x1p[:, ds(own0 + i * sub, sub)] + x1_in[:, cs]).astype(BF16)
        x1s[:, cs] = act
        x1_user[i].start()

        @pl.when(diag)
        def _():
            mine(x1t, y, i)[...] = act
            x1_fwd[0, i].start()

        @pl.when(off)
        def _():
            x1_col[i].start()

    g_load.wait()
    w2_load.wait()
    gbt[...] = g_v[...].astype(BF16)
    dyt[...] = dot(w2_v[...], gbt[...], TN).astype(BF16)

    for i in range(2):
        backward(peer_cols + i * half)
        dz_d2d.append(rcopy(dzp.at[:, ds(peer_cols + i * half, half)], dz_in.at[:, pl.ds(i * half, half)], DZD_S, DZD_R, peer))
        dz_d2d[-1].start()
        sum_x1(i)
    backward(my_cols)
    sum_x1(2)
    backward(my_cols + half)
    wait_recv(dz_in, DZD_R)
    dz_s[...] = dzp[:, ds(my_cols + (1 - x) * half, half)] + dz_in[:, ds((1 - x) * half, half)]
    sum_x1(3)
    dz_x_copies = []
    for i in range(SUBS):
        cs = pl.ds(i * sub, sub)
        dz_x_copies.append(rcopy(dz_s.at[:, cs], dz_x.at[:, cs], DZX_S, DZX_R + i // (SUBS - 1), xn))

    def send_dz(role):
        @pl.when(role)
        def _():
            for copy in dz_x_copies:
                copy.start()

    send_dz(off)
    w1_load.wait()

    def hidden(start, size):
        cs = ds(start, size)
        z1t[:, cs] = jnp.maximum(dot(w1_v[...], x1t[:, cs], TN), 0.0).astype(BF16)

    halves = (y * half, (1 - y) * half)

    def own_piece(i):
        @pl.when(off)
        def _():
            wait_recv(mine(x1t, y, i), X1G_R + 4 * y + i)
            x1_fwd[0, i].start()

        wait_recv(mine(x1t, 1 - y, i), X1G_R + 4 * (1 - y) + i)
        x1_fwd[1, i].start()
        for h in halves:
            hidden(my_cols + h + i * sub, sub)

    def peer_piece(i):
        wait_recv(x1t.at[:, pl.ds(0, 2 * sub)], X1D_R + i)
        for h in halves:
            hidden(peer_cols + h + i * sub, sub)

    def part_x2(rs, block, group):
        total = None
        for h in halves:
            cs = ds(block + h + group * quarter, quarter)
            part = dot(z1t[:, cs], a_v[rs, cs], NT)
            total = part if total is None else total + part
        return total

    own_piece(0)
    send_dz(diag)
    own_piece(1)
    peer_piece(0)
    peer_piece(1)
    x2p[:, a_rows[0]] = part_x2(a_rows[0], my_cols, 0) + part_x2(a_rows[0], peer_cols, 0)
    own_piece(2)
    x2p[:, a_rows[1]] = part_x2(a_rows[1], my_cols, 0) + part_x2(a_rows[1], peer_cols, 0)
    own_piece(3)
    peer_piece(2)
    x2p[:, a_rows[0]] += part_x2(a_rows[0], my_cols, 1)
    peer_piece(3)
    x2_y = []
    for j in range(SUBS):
        rs = ds(other0 + j * sub, sub)
        more = part_x2(rs, peer_cols, 1)
        if j >= 2:
            more = more + part_x2(rs, my_cols, 1)
        x2p[:, rs] += more
        x2_y.append(rcopy(x2p.at[:, rs], x2_in.at[:, pl.ds(j * sub, sub)], X2Y_S, X2Y_R + j // (SUBS - 1), yn))
        x2_y[-1].start()
    for rs in a_rows[2:]:
        x2p[:, rs] = dot(z1t[...], a_v[rs, :], NT)

    dw1 = None
    for i in range(SUBS):
        if i == 0:
            wait_recv(dz_x.at[:, pl.ds(0, half - sub)], DZX_R)
        if i == SUBS - 1:
            wait_recv(dz_x.at[:, pl.ds(0, sub)], DZX_R + 1)
        cs = ds(my_cols + x * half + i * sub, sub)
        d_hidden = (dzp[:, cs] + dz_in[:, ds(x * half + i * sub, sub)]) + dz_x[:, pl.ds(i * sub, sub)]
        d_pre = jnp.where(z1t[:, cs].astype(F32) > 0.0, d_hidden, 0.0).astype(BF16)
        part = dot(x1t[:, cs], d_pre, NT)
        dw1 = part if dw1 is None else dw1 + part
    one_p[pl.ds(0, feat_in)] = dw1
    one_p[pl.ds(feat_in, one_p.shape[0] - feat_in)] = jnp.zeros((one_p.shape[0] - feat_in, one_p.shape[1]), F32)

    n_one = one_p.shape[0] // 2
    one_a = rcopy(one_p.at[ds((1 - c) * n_one, n_one, 8)], one_in, ONE_S, ONE_R, peer)
    one_a.start()
    one_a.wait_recv()
    one_s[...] = one_p[ds(c * n_one, n_one, 8)] + one_in[...]
    one_b = rcopy(one_s, one_x, ONE_S + 1, ONE_R + 1, xn)
    one_b.start()
    one_b.wait_recv()
    one_sx[...] = one_s[...] + one_x[...]
    one_c = rcopy(one_sx, one_y, ONE_S + 2, ONE_R + 2, yn)
    one_c.start()

    dw2 = None
    for i in range(SUBS):
        if i == 0:
            wait_recv(x2_in.at[:, pl.ds(0, half - sub)], X2Y_R)
        if i == SUBS - 1:
            wait_recv(x2_in.at[:, pl.ds(0, sub)], X2Y_R + 1)
        rs = ds(own0 + i * sub, sub)
        act = (x2p[:, rs] + x2_in[:, pl.ds(i * sub, sub)]).astype(BF16)
        part = dot(gbt[:, rs], act, NT)
        dw2 = part if dw2 is None else dw2 + part
    two_p[pl.ds(0, classes)] = dw2
    two_p[pl.ds(classes, two_p.shape[0] - classes)] = jnp.zeros((two_p.shape[0] - classes, two_p.shape[1]), F32)

    n_two = two_p.shape[0] // 2
    chip = 2 * x + y
    two_a = rcopy(two_p.at[ds((1 - c) * n_two, n_two, 8)], two_in, TWO_S, TWO_R, peer)
    two_a.start()
    one_c.wait_recv()
    one_mine = ds(c * n_one, n_one, 8)
    one_tot[one_mine] = one_sx[...] + one_y[...]
    one_d = rcopy(one_tot.at[one_mine], one_tot.at[one_mine], ONE_S + 3, ONE_R + 3, peer)
    one_d.start()
    two_a.wait_recv()
    two_all[chip] = two_p[ds(c * n_two, n_two, 8)] + two_in[...]
    two_b = [rcopy(two_all.at[chip], two_all.at[chip], TWO_S + 1, TWO_R + 1, dev) for dev in (opp, xn, yn)]
    for copy in two_b:
        copy.start()
    one_d.wait_recv()
    dw1_store = pltpu.make_async_copy(one_tot, dw1_out, l_sem.at[6])
    dw1_store.start()
    wait_recv(two_all.at[pl.ds(0, 3)], TWO_R + 1)
    two_mine = ds(c * n_two, n_two, 8)
    two_tot[two_mine] = (two_all[0] + two_all[1]) + (two_all[2] + two_all[3])
    two_c = rcopy(two_tot.at[two_mine], two_tot.at[two_mine], TWO_S + 2, TWO_R + 2, peer)
    two_c.start()
    two_c.wait_recv()
    dw2_store = pltpu.make_async_copy(two_tot, dw2t_out, l_sem.at[7])
    dw2_store.start()

    wait_send(hs, H_S)
    wait_send(ht.at[:, pl.ds(0, rows)], HT_S)
    wait_send(x1_in, X1Y_S)
    wait_send(x1s, X1U_S)

    @pl.when(off)
    def _():
        wait_send(x1s, X1C_S)

    wait_send(x1t.at[:, pl.ds(0, rows)], X1D_S)
    wait_send(dz_in, DZD_S)
    wait_send(dz_s, DZX_S)
    wait_send(x2_in, X2Y_S)
    for copy in (one_a, one_b, one_c, one_d, two_a, two_c):
        copy.wait_send()
    wait_send(two_all.at[pl.ds(0, 3)], TWO_S + 1)
    dw1_store.wait()
    dw2_store.wait()


def finish_kernel(one, two, dw1, dw2t):
    dw1[...] = one[pl.ds(0, dw1.shape[0])]
    dw2t[...] = two[pl.ds(0, dw2t.shape[0])]


def solution(mesh):
    def local_step(adj, feat, w_one, w_two, grad):
        rows, cols = adj.shape
        feat_in, hidden = w_one.shape
        classes = w_two.shape[1]
        half = rows // 2
        fpad, cpad = -(-feat_in // 16) * 16, -(-classes // 16) * 16
        vmem = pltpu.VMEM
        one_half = vmem((fpad // 2, hidden), F32)
        dw1, dw2t = pl.pallas_call(
            gcn_kernel,
            out_shape=(jax.ShapeDtypeStruct((fpad, hidden), F32), jax.ShapeDtypeStruct((cpad, hidden), F32)),
            in_specs=[pl.BlockSpec(memory_space=pltpu.HBM)] * 5,
            out_specs=(pl.BlockSpec(memory_space=pltpu.HBM), pl.BlockSpec(memory_space=pltpu.HBM)),
            scratch_shapes=[
                vmem((rows, cols), BF16),
                vmem((feat_in, cols), BF16),
                vmem((feat_in, half), BF16),
                vmem((classes, rows), F32),
                vmem((feat_in, hidden), BF16),
                vmem((classes, hidden), BF16),
                vmem((classes, rows), BF16),
                vmem((hidden, rows), BF16),
                vmem((hidden, cols), F32),
                vmem((hidden, rows), F32),
                vmem((hidden, half), F32),
                vmem((hidden, half), F32),
                vmem((feat_in, rows), F32),
                vmem((feat_in, half), F32),
                vmem((feat_in, half), BF16),
                vmem((feat_in, cols), BF16),
                vmem((hidden, cols), BF16),
                vmem((hidden, rows), F32),
                vmem((hidden, half), F32),
                vmem((fpad, hidden), F32),
                *[one_half] * 5,
                vmem((fpad, hidden), F32),
                vmem((cpad, hidden), F32),
                vmem((cpad // 2, hidden), F32),
                vmem((4, cpad // 2, hidden), F32),
                vmem((cpad, hidden), F32),
                pltpu.SemaphoreType.DMA((4,)),
                pltpu.SemaphoreType.DMA((8,)),
                pltpu.SemaphoreType.DMA((N_SEND,)),
                pltpu.SemaphoreType.DMA((N_RECV,)),
            ],
            compiler_params=pltpu.CompilerParams(
                collective_id=0, has_side_effects=True, vmem_limit_bytes=60 * 1024 * 1024),
        )(adj, feat.T, w_one, w_two.T, grad.T)
        dw1, dw2t = pl.pallas_call(
            finish_kernel,
            out_shape=(jax.ShapeDtypeStruct((feat_in, hidden), F32), jax.ShapeDtypeStruct((classes, hidden), F32)),
            in_specs=[pl.BlockSpec(memory_space=vmem)] * 2,
            out_specs=(pl.BlockSpec(memory_space=vmem),) * 2,
        )(dw1, dw2t)
        return dw1, dw2t.T

    return jax.shard_map(
        local_step, mesh=mesh,
        in_specs=(P("rows", "rep"), P("rows", None), P(), P(), P("rows", None)),
        out_specs=(P(), P()), check_vma=False)
```

```python
import jax
import jax.numpy as jnp
from jax import lax
from jax.experimental import pallas as pl
from jax.experimental.pallas import tpu as pltpu
from jax.sharding import PartitionSpec as P

MESH = pl.DeviceIdType.MESH
F32 = jnp.float32
BF16 = jnp.bfloat16
NN = (((1,), (0,)), ((), ()))
NT = (((1,), (1,)), ((), ()))
TN = (((0,), (0,)), ((), ()))
SUBS = 4
H_S, HT_S, X1Y_S, X1U_S, X1C_S, X1D_S, DZD_S, DZX_S, X2Y_S, ONE_S, TWO_S, N_SEND = 0, 1, 2, 3, 4, 5, 6, 7, 8, 9, 13, 16
H_R, HT_R, X1Y_R, X1G_R, X1D_R, DZD_R, DZX_R, X2Y_R, ONE_R, TWO_R, N_RECV = 0, 2, 4, 8, 16, 20, 21, 23, 25, 29, 32


def dot(lhs, rhs, dims):
    return lax.dot_general(lhs, rhs, dims, preferred_element_type=F32)


def ds(start, size, align=128):
    return pl.ds(pl.multiple_of(start, align), size)


def gcn_kernel(
    adj, feat, w_one, w_two, grad, dw1_out, dw2t_out,
    a_v, ht, hs, g_v, w1_v, w2_v, gbt, dyt, dzp, dz_in, dz_s, dz_x,
    x1p, x1_in, x1s, x1t, z1t, x2p, x2_in,
    one_p, one_in, one_s, one_x, one_sx, one_y, one_tot, two_p, two_in, two_all, two_tot,
    a_sem, l_sem, send_sem, recv_sem,
):
    y = lax.axis_index("rep")
    r = lax.axis_index("rows")
    x, c = r // 2, lax.rem(r, 2)
    diag = x == y
    off = jnp.logical_not(diag)
    peer = (y, 2 * x + 1 - c)
    xn = (y, 2 * (1 - x) + c)
    yn = (1 - y, r)
    opp = (1 - y, 2 * (1 - x) + c)
    user = (x, 2 * (1 - x) + c)
    rows, cols = a_v.shape
    half, quarter = rows // 2, rows // 4
    sub = half // SUBS
    feat_in, classes = feat.shape[0], grad.shape[0]
    my_cols, peer_cols = c * rows, (1 - c) * rows

    def rcopy(src, dst, send, recv, dev):
        return pltpu.make_async_remote_copy(
            src_ref=src, dst_ref=dst, send_sem=send_sem.at[send], recv_sem=recv_sem.at[recv],
            device_id=dev, device_id_type=MESH)

    def wait_recv(dst, recv):
        rcopy(dst, dst, 0, recv, peer).wait_recv()

    def wait_send(src, send):
        rcopy(src, src, send, 0, peer).wait_send()

    side = jnp.where(diag, 0, 1)
    hs_loads = [pltpu.make_async_copy(feat.at[:, ds((2 * w + side) * quarter, quarter)],
                                      hs.at[:, pl.ds(w * quarter, quarter)], l_sem.at[4 + w]) for w in range(2)]
    h_load = pltpu.make_async_copy(feat, ht.at[:, ds(my_cols, rows)], l_sem.at[3])
    for load in hs_loads:
        load.start()

    @pl.when(diag)
    def _():
        h_load.start()

    g_load = pltpu.make_async_copy(grad, g_v, l_sem.at[0])
    w1_load = pltpu.make_async_copy(w_one, w1_v, l_sem.at[1])
    w2_load = pltpu.make_async_copy(w_two, w2_v, l_sem.at[2])
    own0, other0 = y * half, (1 - y) * half
    a_rows = [ds(other0, quarter), ds(other0 + quarter, quarter), ds(own0, quarter), ds(own0 + quarter, quarter)]
    a_loads = []
    for i, start in enumerate((other0, other0 + quarter, own0, own0 + quarter)):
        for j in range(2):
            rs = ds(start + j * sub, sub)
            a_loads.append(pltpu.make_async_copy(adj.at[rs], a_v.at[rs], a_sem.at[i]))
    for load in a_loads[:4]:
        load.start()

    def wait_a(i):
        pltpu.make_async_copy(adj.at[a_rows[i]], a_v.at[a_rows[i]], a_sem.at[i]).wait()

    barrier = pltpu.get_barrier_semaphore()
    for dev in (peer, xn, yn, opp):
        pl.semaphore_signal(barrier, inc=1, device_id=dev, device_id_type=MESH)
    pl.semaphore_wait(barrier, 4)

    def h_piece(k):
        return ht.at[:, ds(my_cols + k * quarter, quarter)]

    for w in range(2):
        hs_loads[w].wait()
        rcopy(hs.at[:, pl.ds(w * quarter, quarter)], h_piece(2 * w + side), H_S, H_R + w, user).start()

    for load in a_loads[4:]:
        load.start()
    for load in (g_load, w1_load, w2_load):
        load.start()
    def h_wave(w, start):
        return ht.at[:, ds(start + w * half, half)]

    h_fwd = [rcopy(h_wave(w, my_cols), h_wave(w, my_cols), HT_S, HT_R + w, peer) for w in range(2)]

    @pl.when(diag)
    def _():
        h_load.wait()
        for w in range(2):
            h_fwd[w].start()

    x1_y = []

    def add_x1(rs, cs, first=False):
        part = dot(ht[:, cs], a_v[rs, cs], NT)
        x1p[:, rs] = part if first else x1p[:, rs] + part

    for j in range(SUBS):
        x1_y.append(rcopy(x1p.at[:, ds(other0 + j * sub, sub)], x1_in.at[:, pl.ds(j * sub, sub)], X1Y_S, X1Y_R + j, yn))

    def send_x1(subs, role):
        @pl.when(role)
        def _():
            for j in subs:
                x1_y[j].start()

    def forward_h(w):
        @pl.when(off)
        def _():
            wait_recv(h_wave(w, my_cols), H_R + w)
            h_fwd[w].start()

    waves = [(ds(my_cols + w * half, half), ds(peer_cols + w * half, half)) for w in range(2)]
    forward_h(0)
    for i in range(2):
        wait_a(i)
        add_x1(a_rows[i], waves[0][0], True)
    h_fwd[0].wait_recv()
    for i in range(2):
        add_x1(a_rows[i], waves[0][1])
    forward_h(1)
    add_x1(a_rows[0], waves[1][0])
    h_fwd[1].wait_recv()
    for j in range(2):
        add_x1(ds(other0 + j * sub, sub), waves[1][1])
        send_x1((j,), off)
    add_x1(a_rows[1], waves[1][0])
    add_x1(a_rows[1], waves[1][1])
    send_x1(range(SUBS), diag)
    send_x1((2, 3), off)
    for i in range(2, 4):
        wait_a(i)
        x1p[:, a_rows[i]] = dot(ht[...], a_v[a_rows[i], :], NT)

    dz_d2d = []

    def backward(start):
        cs = ds(start, half)
        dzp[:, cs] = dot(dyt[...], a_v[:, cs], NN)

    def mine(ref, h, i):
        return ref.at[:, ds(my_cols + h * half + i * sub, sub)]

    x1_fwd = {(h, i): rcopy(mine(x1t, hv, i), mine(x1t, hv, i), X1D_S, X1D_R + i, peer)
              for h, hv in ((0, y), (1, 1 - y)) for i in range(SUBS)}
    x1_user, x1_col = [], []

    for i in range(SUBS):
        piece = x1s.at[:, pl.ds(i * sub, sub)]
        x1_user.append(rcopy(piece, mine(x1t, y, i), X1U_S, X1G_R + 4 * y + i, user))
        x1_col.append(rcopy(piece, mine(x1t, y, i), X1C_S, X1G_R + 4 * y + i, yn))

    def sum_x1(i):
        x1_y[i].wait_recv()
        cs = pl.ds(i * sub, sub)
        act = (x1p[:, ds(own0 + i * sub, sub)] + x1_in[:, cs]).astype(BF16)
        x1s[:, cs] = act
        x1_user[i].start()

        @pl.when(diag)
        def _():
            mine(x1t, y, i)[...] = act
            x1_fwd[0, i].start()

        @pl.when(off)
        def _():
            x1_col[i].start()

    g_load.wait()
    w2_load.wait()
    gbt[...] = g_v[...].astype(BF16)
    dyt[...] = dot(w2_v[...], gbt[...], TN).astype(BF16)

    for i in range(2):
        backward(peer_cols + i * half)
        dz_d2d.append(rcopy(dzp.at[:, ds(peer_cols + i * half, half)], dz_in.at[:, pl.ds(i * half, half)], DZD_S, DZD_R, peer))
        dz_d2d[-1].start()
        sum_x1(i)
    backward(my_cols)
    sum_x1(2)
    backward(my_cols + half)
    wait_recv(dz_in, DZD_R)
    dz_s[...] = dzp[:, ds(my_cols + (1 - x) * half, half)] + dz_in[:, ds((1 - x) * half, half)]
    sum_x1(3)
    dz_x_copies = []
    for i in range(SUBS):
        cs = pl.ds(i * sub, sub)
        dz_x_copies.append(rcopy(dz_s.at[:, cs], dz_x.at[:, cs], DZX_S, DZX_R + i // (SUBS - 1), xn))

    def send_dz(role):
        @pl.when(role)
        def _():
            for copy in dz_x_copies:
                copy.start()

    send_dz(off)
    w1_load.wait()

    def hidden(start, size):
        cs = ds(start, size)
        z1t[:, cs] = jnp.maximum(dot(w1_v[...], x1t[:, cs], TN), 0.0).astype(BF16)

    halves = (y * half, (1 - y) * half)

    def own_piece(i):
        @pl.when(off)
        def _():
            wait_recv(mine(x1t, y, i), X1G_R + 4 * y + i)
            x1_fwd[0, i].start()

        wait_recv(mine(x1t, 1 - y, i), X1G_R + 4 * (1 - y) + i)
        x1_fwd[1, i].start()
        for h in halves:
            hidden(my_cols + h + i * sub, sub)

    def peer_piece(i):
        wait_recv(x1t.at[:, pl.ds(0, 2 * sub)], X1D_R + i)
        for h in halves:
            hidden(peer_cols + h + i * sub, sub)

    def part_x2(rs, block, group):
        total = None
        for h in halves:
            cs = ds(block + h + group * quarter, quarter)
            part = dot(z1t[:, cs], a_v[rs, cs], NT)
            total = part if total is None else total + part
        return total

    own_piece(0)
    send_dz(diag)
    own_piece(1)
    peer_piece(0)
    peer_piece(1)
    x2p[:, a_rows[0]] = part_x2(a_rows[0], my_cols, 0) + part_x2(a_rows[0], peer_cols, 0)
    own_piece(2)
    own_piece(3)
    peer_piece(2)
    x2p[:, a_rows[0]] += part_x2(a_rows[0], my_cols, 1)
    peer_piece(3)
    x2_y = []
    for j in range(SUBS):
        rs = ds(other0 + j * sub, sub)
        if j < 2:
            x2p[:, rs] += part_x2(rs, peer_cols, 1)
        if j == 2:
            x2p[:, a_rows[1]] = dot(z1t[...], a_v[a_rows[1], :], NT)
        x2_y.append(rcopy(x2p.at[:, rs], x2_in.at[:, pl.ds(j * sub, sub)], X2Y_S, X2Y_R + j // (SUBS - 1), yn))
        x2_y[-1].start()
    for rs in a_rows[2:]:
        x2p[:, rs] = dot(z1t[...], a_v[rs, :], NT)

    dw1 = None
    for i in range(SUBS):
        if i == 0:
            wait_recv(dz_x.at[:, pl.ds(0, half - sub)], DZX_R)
        if i == SUBS - 1:
            wait_recv(dz_x.at[:, pl.ds(0, sub)], DZX_R + 1)
        cs = ds(my_cols + x * half + i * sub, sub)
        d_hidden = (dzp[:, cs] + dz_in[:, ds(x * half + i * sub, sub)]) + dz_x[:, pl.ds(i * sub, sub)]
        d_pre = jnp.where(z1t[:, cs].astype(F32) > 0.0, d_hidden, 0.0).astype(BF16)
        part = dot(x1t[:, cs], d_pre, NT)
        dw1 = part if dw1 is None else dw1 + part
    one_p[pl.ds(0, feat_in)] = dw1
    one_p[pl.ds(feat_in, one_p.shape[0] - feat_in)] = jnp.zeros((one_p.shape[0] - feat_in, one_p.shape[1]), F32)

    n_one = one_p.shape[0] // 2
    one_a = rcopy(one_p.at[ds((1 - c) * n_one, n_one, 8)], one_in, ONE_S, ONE_R, peer)
    one_a.start()
    one_a.wait_recv()
    one_s[...] = one_p[ds(c * n_one, n_one, 8)] + one_in[...]
    one_b = rcopy(one_s, one_x, ONE_S + 1, ONE_R + 1, xn)
    one_b.start()
    one_b.wait_recv()
    one_sx[...] = one_s[...] + one_x[...]
    one_c = rcopy(one_sx, one_y, ONE_S + 2, ONE_R + 2, yn)
    one_c.start()

    dw2 = None
    for i in range(SUBS):
        if i == 0:
            wait_recv(x2_in.at[:, pl.ds(0, half - sub)], X2Y_R)
        if i == SUBS - 1:
            wait_recv(x2_in.at[:, pl.ds(0, sub)], X2Y_R + 1)
        rs = ds(own0 + i * sub, sub)
        act = (x2p[:, rs] + x2_in[:, pl.ds(i * sub, sub)]).astype(BF16)
        part = dot(gbt[:, rs], act, NT)
        dw2 = part if dw2 is None else dw2 + part
    two_p[pl.ds(0, classes)] = dw2
    two_p[pl.ds(classes, two_p.shape[0] - classes)] = jnp.zeros((two_p.shape[0] - classes, two_p.shape[1]), F32)

    n_two = two_p.shape[0] // 2
    chip = 2 * x + y
    two_a = rcopy(two_p.at[ds((1 - c) * n_two, n_two, 8)], two_in, TWO_S, TWO_R, peer)
    two_a.start()
    two_a.wait_recv()
    two_all[chip] = two_p[ds(c * n_two, n_two, 8)] + two_in[...]
    two_b = [rcopy(two_all.at[chip], two_all.at[chip], TWO_S + 1, TWO_R + 1, dev) for dev in (opp, xn, yn)]
    for copy in two_b:
        copy.start()
    one_c.wait_recv()
    one_mine = ds(c * n_one, n_one, 8)
    one_tot[one_mine] = one_sx[...] + one_y[...]
    one_d = rcopy(one_tot.at[one_mine], one_tot.at[one_mine], ONE_S + 3, ONE_R + 3, peer)
    one_d.start()
    one_d.wait_recv()
    dw1_store = pltpu.make_async_copy(one_tot, dw1_out, l_sem.at[6])
    dw1_store.start()
    wait_recv(two_all.at[pl.ds(0, 3)], TWO_R + 1)
    two_mine = ds(c * n_two, n_two, 8)
    two_tot[two_mine] = (two_all[0] + two_all[1]) + (two_all[2] + two_all[3])
    two_c = rcopy(two_tot.at[two_mine], two_tot.at[two_mine], TWO_S + 2, TWO_R + 2, peer)
    two_c.start()
    two_c.wait_recv()
    dw2_store = pltpu.make_async_copy(two_tot, dw2t_out, l_sem.at[7])
    dw2_store.start()

    wait_send(hs, H_S)
    wait_send(ht.at[:, pl.ds(0, rows)], HT_S)
    wait_send(x1_in, X1Y_S)
    wait_send(x1s, X1U_S)

    @pl.when(off)
    def _():
        wait_send(x1s, X1C_S)

    wait_send(x1t.at[:, pl.ds(0, rows)], X1D_S)
    wait_send(dz_in, DZD_S)
    wait_send(dz_s, DZX_S)
    wait_send(x2_in, X2Y_S)
    for copy in (one_a, one_b, one_c, one_d, two_a, two_c):
        copy.wait_send()
    wait_send(two_all.at[pl.ds(0, 3)], TWO_S + 1)
    dw1_store.wait()
    dw2_store.wait()


def finish_kernel(one, two, dw1, dw2t):
    dw1[...] = one[pl.ds(0, dw1.shape[0])]
    dw2t[...] = two[pl.ds(0, dw2t.shape[0])]


def solution(mesh):
    def local_step(adj, feat, w_one, w_two, grad):
        rows, cols = adj.shape
        feat_in, hidden = w_one.shape
        classes = w_two.shape[1]
        half = rows // 2
        fpad, cpad = -(-feat_in // 16) * 16, -(-classes // 16) * 16
        vmem = pltpu.VMEM
        one_half = vmem((fpad // 2, hidden), F32)
        dw1, dw2t = pl.pallas_call(
            gcn_kernel,
            out_shape=(jax.ShapeDtypeStruct((fpad, hidden), F32), jax.ShapeDtypeStruct((cpad, hidden), F32)),
            in_specs=[pl.BlockSpec(memory_space=pltpu.HBM)] * 5,
            out_specs=(pl.BlockSpec(memory_space=pltpu.HBM), pl.BlockSpec(memory_space=pltpu.HBM)),
            scratch_shapes=[
                vmem((rows, cols), BF16),
                vmem((feat_in, cols), BF16),
                vmem((feat_in, half), BF16),
                vmem((classes, rows), F32),
                vmem((feat_in, hidden), BF16),
                vmem((classes, hidden), BF16),
                vmem((classes, rows), BF16),
                vmem((hidden, rows), BF16),
                vmem((hidden, cols), F32),
                vmem((hidden, rows), F32),
                vmem((hidden, half), F32),
                vmem((hidden, half), F32),
                vmem((feat_in, rows), F32),
                vmem((feat_in, half), F32),
                vmem((feat_in, half), BF16),
                vmem((feat_in, cols), BF16),
                vmem((hidden, cols), BF16),
                vmem((hidden, rows), F32),
                vmem((hidden, half), F32),
                vmem((fpad, hidden), F32),
                *[one_half] * 5,
                vmem((fpad, hidden), F32),
                vmem((cpad, hidden), F32),
                vmem((cpad // 2, hidden), F32),
                vmem((4, cpad // 2, hidden), F32),
                vmem((cpad, hidden), F32),
                pltpu.SemaphoreType.DMA((4,)),
                pltpu.SemaphoreType.DMA((8,)),
                pltpu.SemaphoreType.DMA((N_SEND,)),
                pltpu.SemaphoreType.DMA((N_RECV,)),
            ],
            compiler_params=pltpu.CompilerParams(
                collective_id=0, has_side_effects=True, vmem_limit_bytes=60 * 1024 * 1024),
        )(adj, feat.T, w_one, w_two.T, grad.T)
        dw1, dw2t = pl.pallas_call(
            finish_kernel,
            out_shape=(jax.ShapeDtypeStruct((feat_in, hidden), F32), jax.ShapeDtypeStruct((classes, hidden), F32)),
            in_specs=[pl.BlockSpec(memory_space=vmem)] * 2,
            out_specs=(pl.BlockSpec(memory_space=vmem),) * 2,
        )(dw1, dw2t)
        return dw1, dw2t.T

    return jax.shard_map(
        local_step, mesh=mesh,
        in_specs=(P("rows", "rep"), P("rows", None), P(), P(), P("rows", None)),
        out_specs=(P(), P()), check_vma=False)
```

```python
import jax
import jax.numpy as jnp
from jax import lax
from jax.experimental import pallas as pl
from jax.experimental.pallas import tpu as pltpu
from jax.sharding import PartitionSpec as P

MESH = pl.DeviceIdType.MESH
F32 = jnp.float32
BF16 = jnp.bfloat16
NN = (((1,), (0,)), ((), ()))
NT = (((1,), (1,)), ((), ()))
TN = (((0,), (0,)), ((), ()))
SUBS = 4
H_S, HT_S, X1Y_S, X1U_S, X1C_S, X1D_S, DZD_S, DZX_S, X2Y_S, ONE_S, TWO_S, N_SEND = 0, 1, 2, 3, 4, 5, 6, 7, 8, 9, 13, 15
H_R, HT_R, X1Y_R, X1G_R, X1D_R, DZD_R, DZX_R, X2Y_R, ONE_R, TWO_R, N_RECV = 0, 2, 4, 8, 16, 20, 21, 23, 25, 29, 31


def dot(lhs, rhs, dims):
    return lax.dot_general(lhs, rhs, dims, preferred_element_type=F32)


def ds(start, size, align=128):
    return pl.ds(pl.multiple_of(start, align), size)


def gcn_kernel(
    adj, feat, w_one, w_two, grad, dw1_out, dw2t_out,
    a_v, ht, hs, g_v, w1_v, w2_v, gbt, dyt, dzp, dz_in, dz_s, dz_x,
    x1p, x1_in, x1s, x1t, z1t, x2p, x2_in,
    one_p, one_in, one_s, one_x, one_sx, one_y, one_tot, two_p, two_all, two_tot,
    a_sem, l_sem, send_sem, recv_sem,
):
    y = lax.axis_index("rep")
    r = lax.axis_index("rows")
    x, c = r // 2, lax.rem(r, 2)
    diag = x == y
    off = jnp.logical_not(diag)
    peer = (y, 2 * x + 1 - c)
    xn = (y, 2 * (1 - x) + c)
    yn = (1 - y, r)
    opp = (1 - y, 2 * (1 - x) + c)
    far = [(yy, 2 * xx + cc) for yy, xx in ((1 - y, 1 - x), (y, 1 - x), (1 - y, x)) for cc in (c, 1 - c)]
    user = (x, 2 * (1 - x) + c)
    rows, cols = a_v.shape
    half, quarter = rows // 2, rows // 4
    sub = half // SUBS
    feat_in, classes = feat.shape[0], grad.shape[0]
    my_cols, peer_cols = c * rows, (1 - c) * rows

    def rcopy(src, dst, send, recv, dev):
        return pltpu.make_async_remote_copy(
            src_ref=src, dst_ref=dst, send_sem=send_sem.at[send], recv_sem=recv_sem.at[recv],
            device_id=dev, device_id_type=MESH)

    def wait_recv(dst, recv):
        rcopy(dst, dst, 0, recv, peer).wait_recv()

    def wait_send(src, send):
        rcopy(src, src, send, 0, peer).wait_send()

    side = jnp.where(diag, 0, 1)
    hs_loads = [pltpu.make_async_copy(feat.at[:, ds((2 * w + side) * quarter, quarter)],
                                      hs.at[:, pl.ds(w * quarter, quarter)], l_sem.at[4 + w]) for w in range(2)]
    h_load = pltpu.make_async_copy(feat, ht.at[:, ds(my_cols, rows)], l_sem.at[3])
    for load in hs_loads:
        load.start()

    @pl.when(diag)
    def _():
        h_load.start()

    g_load = pltpu.make_async_copy(grad, g_v, l_sem.at[0])
    w1_load = pltpu.make_async_copy(w_one, w1_v, l_sem.at[1])
    w2_load = pltpu.make_async_copy(w_two, w2_v, l_sem.at[2])
    own0, other0 = y * half, (1 - y) * half
    a_rows = [ds(other0, quarter), ds(other0 + quarter, quarter), ds(own0, quarter), ds(own0 + quarter, quarter)]
    a_loads = []
    for i, start in enumerate((other0, other0 + quarter, own0, own0 + quarter)):
        for j in range(2):
            rs = ds(start + j * sub, sub)
            a_loads.append(pltpu.make_async_copy(adj.at[rs], a_v.at[rs], a_sem.at[i]))
    for load in a_loads[:4]:
        load.start()

    def wait_a(i):
        pltpu.make_async_copy(adj.at[a_rows[i]], a_v.at[a_rows[i]], a_sem.at[i]).wait()

    barrier = pltpu.get_barrier_semaphore()
    for dev in (peer, *far):
        pl.semaphore_signal(barrier, inc=1, device_id=dev, device_id_type=MESH)
    pl.semaphore_wait(barrier, 7)

    def h_piece(k):
        return ht.at[:, ds(my_cols + k * quarter, quarter)]

    for w in range(2):
        hs_loads[w].wait()
        rcopy(hs.at[:, pl.ds(w * quarter, quarter)], h_piece(2 * w + side), H_S, H_R + w, user).start()

    for load in a_loads[4:]:
        load.start()
    for load in (g_load, w1_load, w2_load):
        load.start()
    def h_wave(w, start):
        return ht.at[:, ds(start + w * half, half)]

    h_fwd = [rcopy(h_wave(w, my_cols), h_wave(w, my_cols), HT_S, HT_R + w, peer) for w in range(2)]

    @pl.when(diag)
    def _():
        h_load.wait()
        for w in range(2):
            h_fwd[w].start()

    x1_y = []

    def add_x1(rs, cs, first=False):
        part = dot(ht[:, cs], a_v[rs, cs], NT)
        x1p[:, rs] = part if first else x1p[:, rs] + part

    for j in range(SUBS):
        x1_y.append(rcopy(x1p.at[:, ds(other0 + j * sub, sub)], x1_in.at[:, pl.ds(j * sub, sub)], X1Y_S, X1Y_R + j, yn))

    def send_x1(subs, role):
        @pl.when(role)
        def _():
            for j in subs:
                x1_y[j].start()

    def forward_h(w):
        @pl.when(off)
        def _():
            wait_recv(h_wave(w, my_cols), H_R + w)
            h_fwd[w].start()

    waves = [(ds(my_cols + w * half, half), ds(peer_cols + w * half, half)) for w in range(2)]
    forward_h(0)
    for i in range(2):
        wait_a(i)
        add_x1(a_rows[i], waves[0][0], True)
    h_fwd[0].wait_recv()
    for i in range(2):
        add_x1(a_rows[i], waves[0][1])
    forward_h(1)
    add_x1(a_rows[0], waves[1][0])
    h_fwd[1].wait_recv()
    for j in range(2):
        add_x1(ds(other0 + j * sub, sub), waves[1][1])
        send_x1((j,), off)
    add_x1(a_rows[1], waves[1][0])
    add_x1(a_rows[1], waves[1][1])
    send_x1(range(SUBS), diag)
    send_x1((2, 3), off)
    for i in range(2, 4):
        wait_a(i)
        x1p[:, a_rows[i]] = dot(ht[...], a_v[a_rows[i], :], NT)

    dz_d2d = []

    def backward(start):
        cs = ds(start, half)
        dzp[:, cs] = dot(dyt[...], a_v[:, cs], NN)

    def mine(ref, h, i):
        return ref.at[:, ds(my_cols + h * half + i * sub, sub)]

    x1_fwd = {(h, i): rcopy(mine(x1t, hv, i), mine(x1t, hv, i), X1D_S, X1D_R + i, peer)
              for h, hv in ((0, y), (1, 1 - y)) for i in range(SUBS)}
    x1_user, x1_col = [], []

    for i in range(SUBS):
        piece = x1s.at[:, pl.ds(i * sub, sub)]
        x1_user.append(rcopy(piece, mine(x1t, y, i), X1U_S, X1G_R + 4 * y + i, user))
        x1_col.append(rcopy(piece, mine(x1t, y, i), X1C_S, X1G_R + 4 * y + i, yn))

    def sum_x1(i):
        x1_y[i].wait_recv()
        cs = pl.ds(i * sub, sub)
        act = (x1p[:, ds(own0 + i * sub, sub)] + x1_in[:, cs]).astype(BF16)
        x1s[:, cs] = act
        x1_user[i].start()

        @pl.when(diag)
        def _():
            mine(x1t, y, i)[...] = act
            x1_fwd[0, i].start()

        @pl.when(off)
        def _():
            x1_col[i].start()

    g_load.wait()
    w2_load.wait()
    gbt[...] = g_v[...].astype(BF16)
    dyt[...] = dot(w2_v[...], gbt[...], TN).astype(BF16)

    for i in range(2):
        backward(peer_cols + i * half)
        dz_d2d.append(rcopy(dzp.at[:, ds(peer_cols + i * half, half)], dz_in.at[:, pl.ds(i * half, half)], DZD_S, DZD_R, peer))
        dz_d2d[-1].start()
        sum_x1(i)
    backward(my_cols)
    sum_x1(2)
    backward(my_cols + half)
    wait_recv(dz_in, DZD_R)
    dz_s[...] = dzp[:, ds(my_cols + (1 - x) * half, half)] + dz_in[:, ds((1 - x) * half, half)]
    sum_x1(3)
    dz_x_copies = []
    for i in range(SUBS):
        cs = pl.ds(i * sub, sub)
        dz_x_copies.append(rcopy(dz_s.at[:, cs], dz_x.at[:, cs], DZX_S, DZX_R + i // (SUBS - 1), xn))

    def send_dz(role):
        @pl.when(role)
        def _():
            for copy in dz_x_copies:
                copy.start()

    send_dz(off)
    w1_load.wait()

    def hidden(start, size):
        cs = ds(start, size)
        z1t[:, cs] = jnp.maximum(dot(w1_v[...], x1t[:, cs], TN), 0.0).astype(BF16)

    halves = (y * half, (1 - y) * half)

    def own_piece(i):
        @pl.when(off)
        def _():
            wait_recv(mine(x1t, y, i), X1G_R + 4 * y + i)
            x1_fwd[0, i].start()

        wait_recv(mine(x1t, 1 - y, i), X1G_R + 4 * (1 - y) + i)
        x1_fwd[1, i].start()
        for h in halves:
            hidden(my_cols + h + i * sub, sub)

    def peer_piece(i):
        wait_recv(x1t.at[:, pl.ds(0, 2 * sub)], X1D_R + i)
        for h in halves:
            hidden(peer_cols + h + i * sub, sub)

    def part_x2(rs, block, group):
        total = None
        for h in halves:
            cs = ds(block + h + group * quarter, quarter)
            part = dot(z1t[:, cs], a_v[rs, cs], NT)
            total = part if total is None else total + part
        return total

    own_piece(0)
    own_piece(1)
    send_dz(diag)
    peer_piece(0)
    peer_piece(1)
    x2p[:, a_rows[0]] = part_x2(a_rows[0], my_cols, 0) + part_x2(a_rows[0], peer_cols, 0)
    own_piece(2)
    own_piece(3)
    peer_piece(2)
    x2p[:, a_rows[0]] += part_x2(a_rows[0], my_cols, 1)
    peer_piece(3)
    x2_y = []
    for j in range(SUBS):
        rs = ds(other0 + j * sub, sub)
        if j < 2:
            x2p[:, rs] += part_x2(rs, peer_cols, 1)
        if j == 2:
            x2p[:, a_rows[1]] = dot(z1t[...], a_v[a_rows[1], :], NT)
        x2_y.append(rcopy(x2p.at[:, rs], x2_in.at[:, pl.ds(j * sub, sub)], X2Y_S, X2Y_R + j // (SUBS - 1), yn))
        x2_y[-1].start()
    for rs in a_rows[2:]:
        x2p[:, rs] = dot(z1t[...], a_v[rs, :], NT)

    dw1 = None
    for i in range(SUBS):
        if i == 0:
            wait_recv(dz_x.at[:, pl.ds(0, half - sub)], DZX_R)
        if i == SUBS - 1:
            wait_recv(dz_x.at[:, pl.ds(0, sub)], DZX_R + 1)
        cs = ds(my_cols + x * half + i * sub, sub)
        d_hidden = (dzp[:, cs] + dz_in[:, ds(x * half + i * sub, sub)]) + dz_x[:, pl.ds(i * sub, sub)]
        d_pre = jnp.where(z1t[:, cs].astype(F32) > 0.0, d_hidden, 0.0).astype(BF16)
        part = dot(x1t[:, cs], d_pre, NT)
        dw1 = part if dw1 is None else dw1 + part
    one_p[pl.ds(0, feat_in)] = dw1
    one_p[pl.ds(feat_in, one_p.shape[0] - feat_in)] = jnp.zeros((one_p.shape[0] - feat_in, one_p.shape[1]), F32)

    n_one = one_p.shape[0] // 2
    one_a = rcopy(one_p.at[ds((1 - c) * n_one, n_one, 8)], one_in, ONE_S, ONE_R, peer)
    one_a.start()
    one_a.wait_recv()
    one_s[...] = one_p[ds(c * n_one, n_one, 8)] + one_in[...]
    one_b = rcopy(one_s, one_x, ONE_S + 1, ONE_R + 1, xn)
    one_b.start()
    one_c = rcopy(one_sx, one_y, ONE_S + 2, ONE_R + 2, yn)

    def send_one_y(role):
        @pl.when(role)
        def _():
            one_b.wait_recv()
            one_sx[...] = one_s[...] + one_x[...]
            one_c.start()

    send_one_y(off)

    dw2 = None
    for i in range(SUBS):
        if i == 0:
            wait_recv(x2_in.at[:, pl.ds(0, half - sub)], X2Y_R)
        if i == SUBS - 1:
            wait_recv(x2_in.at[:, pl.ds(0, sub)], X2Y_R + 1)
        rs = ds(own0 + i * sub, sub)
        act = (x2p[:, rs] + x2_in[:, pl.ds(i * sub, sub)]).astype(BF16)
        part = dot(gbt[:, rs], act, NT)
        dw2 = part if dw2 is None else dw2 + part
    two_p[pl.ds(0, classes)] = dw2
    two_p[pl.ds(classes, two_p.shape[0] - classes)] = jnp.zeros((two_p.shape[0] - classes, two_p.shape[1]), F32)

    n_two = two_p.shape[0] // 2
    me = 2 * (2 * x + y) + c
    two_mine, two_peer = ds(c * n_two, n_two, 8), ds((1 - c) * n_two, n_two, 8)
    for k, dev in enumerate((*far, peer)):
        rows_k = two_mine if k < 6 and k % 2 == 0 else two_peer
        rcopy(two_p.at[rows_k], two_all.at[me], TWO_S, TWO_R, dev).start()
    two_all[me] = two_p[two_mine]
    send_one_y(diag)
    one_c.wait_recv()
    one_mine = ds(c * n_one, n_one, 8)
    one_tot[one_mine] = one_sx[...] + one_y[...]
    one_d = rcopy(one_tot.at[one_mine], one_tot.at[one_mine], ONE_S + 3, ONE_R + 3, peer)
    one_d.start()
    wait_recv(two_all.at[pl.ds(0, 7)], TWO_R)
    pairs = [two_all[2 * k] + two_all[2 * k + 1] for k in range(4)]
    two_tot[two_mine] = (pairs[0] + pairs[1]) + (pairs[2] + pairs[3])
    two_c = rcopy(two_tot.at[two_mine], two_tot.at[two_mine], TWO_S + 1, TWO_R + 1, peer)
    two_c.start()
    one_d.wait_recv()
    dw1_store = pltpu.make_async_copy(one_tot, dw1_out, l_sem.at[6])
    dw1_store.start()
    two_c.wait_recv()
    dw2_store = pltpu.make_async_copy(two_tot, dw2t_out, l_sem.at[7])
    dw2_store.start()

    wait_send(hs, H_S)
    wait_send(ht.at[:, pl.ds(0, rows)], HT_S)
    wait_send(x1_in, X1Y_S)
    wait_send(x1s, X1U_S)

    @pl.when(off)
    def _():
        wait_send(x1s, X1C_S)

    wait_send(x1t.at[:, pl.ds(0, rows)], X1D_S)
    wait_send(dz_in, DZD_S)
    wait_send(dz_s, DZX_S)
    wait_send(x2_in, X2Y_S)
    for copy in (one_a, one_b, one_c, one_d, two_c):
        copy.wait_send()
    wait_send(two_all.at[pl.ds(0, 7)], TWO_S)
    dw1_store.wait()
    dw2_store.wait()


def finish_kernel(one, two, dw1, dw2t):
    dw1[...] = one[pl.ds(0, dw1.shape[0])]
    dw2t[...] = two[pl.ds(0, dw2t.shape[0])]


def solution(mesh):
    def local_step(adj, feat, w_one, w_two, grad):
        rows, cols = adj.shape
        feat_in, hidden = w_one.shape
        classes = w_two.shape[1]
        half = rows // 2
        fpad, cpad = -(-feat_in // 16) * 16, -(-classes // 16) * 16
        vmem = pltpu.VMEM
        one_half = vmem((fpad // 2, hidden), F32)
        dw1, dw2t = pl.pallas_call(
            gcn_kernel,
            out_shape=(jax.ShapeDtypeStruct((fpad, hidden), F32), jax.ShapeDtypeStruct((cpad, hidden), F32)),
            in_specs=[pl.BlockSpec(memory_space=pltpu.HBM)] * 5,
            out_specs=(pl.BlockSpec(memory_space=pltpu.HBM), pl.BlockSpec(memory_space=pltpu.HBM)),
            scratch_shapes=[
                vmem((rows, cols), BF16),
                vmem((feat_in, cols), BF16),
                vmem((feat_in, half), BF16),
                vmem((classes, rows), F32),
                vmem((feat_in, hidden), BF16),
                vmem((classes, hidden), BF16),
                vmem((classes, rows), BF16),
                vmem((hidden, rows), BF16),
                vmem((hidden, cols), F32),
                vmem((hidden, rows), F32),
                vmem((hidden, half), F32),
                vmem((hidden, half), F32),
                vmem((feat_in, rows), F32),
                vmem((feat_in, half), F32),
                vmem((feat_in, half), BF16),
                vmem((feat_in, cols), BF16),
                vmem((hidden, cols), BF16),
                vmem((hidden, rows), F32),
                vmem((hidden, half), F32),
                vmem((fpad, hidden), F32),
                *[one_half] * 5,
                vmem((fpad, hidden), F32),
                vmem((cpad, hidden), F32),
                vmem((8, cpad // 2, hidden), F32),
                vmem((cpad, hidden), F32),
                pltpu.SemaphoreType.DMA((4,)),
                pltpu.SemaphoreType.DMA((8,)),
                pltpu.SemaphoreType.DMA((N_SEND,)),
                pltpu.SemaphoreType.DMA((N_RECV,)),
            ],
            compiler_params=pltpu.CompilerParams(
                collective_id=0, has_side_effects=True, vmem_limit_bytes=60 * 1024 * 1024),
        )(adj, feat.T, w_one, w_two.T, grad.T)
        dw1, dw2t = pl.pallas_call(
            finish_kernel,
            out_shape=(jax.ShapeDtypeStruct((feat_in, hidden), F32), jax.ShapeDtypeStruct((classes, hidden), F32)),
            in_specs=[pl.BlockSpec(memory_space=vmem)] * 2,
            out_specs=(pl.BlockSpec(memory_space=vmem),) * 2,
        )(dw1, dw2t)
        return dw1, dw2t.T

    return jax.shard_map(
        local_step, mesh=mesh,
        in_specs=(P("rows", "rep"), P("rows", None), P(), P(), P("rows", None)),
        out_specs=(P(), P()), check_vma=False)
```

```python
import jax
import jax.numpy as jnp
from jax import lax
from jax.experimental import pallas as pl
from jax.experimental.pallas import tpu as pltpu
from jax.sharding import PartitionSpec as P

MESH = pl.DeviceIdType.MESH
F32 = jnp.float32
BF16 = jnp.bfloat16
NN = (((1,), (0,)), ((), ()))
NT = (((1,), (1,)), ((), ()))
TN = (((0,), (0,)), ((), ()))
SUBS = 4
H_S, HT_S, X1Y_S, X1U_S, X1C_S, X1D_S, DZD_S, DZX_S, X2Y_S, ONE_S, TWO_S, N_SEND = 0, 1, 2, 3, 4, 5, 6, 7, 8, 9, 13, 15
H_R, HT_R, X1Y_R, X1G_R, X1D_R, DZD_R, DZX_R, X2Y_R, ONE_R, TWO_R, N_RECV = 0, 2, 4, 8, 16, 20, 21, 23, 25, 29, 31


def dot(lhs, rhs, dims):
    return lax.dot_general(lhs, rhs, dims, preferred_element_type=F32)


def ds(start, size, align=128):
    return pl.ds(pl.multiple_of(start, align), size)


def gcn_kernel(
    adj, feat, w_one, w_two, grad, dw1_out, dw2t_out,
    a_v, ht, hs, g_v, w1_v, w2_v, gbt, dyt, dzp, dz_in, dz_s, dz_x,
    x1p, x1_in, x1s, x1t, z1t, x2p, x2_in,
    one_p, one_in, one_s, one_x, one_sx, one_y, one_tot, two_p, two_all, two_tot,
    a_sem, l_sem, send_sem, recv_sem,
):
    y = lax.axis_index("rep")
    r = lax.axis_index("rows")
    x, c = r // 2, lax.rem(r, 2)
    diag = x == y
    off = jnp.logical_not(diag)
    peer = (y, 2 * x + 1 - c)
    xn = (y, 2 * (1 - x) + c)
    yn = (1 - y, r)
    opp = (1 - y, 2 * (1 - x) + c)
    far = [(yy, 2 * xx + cc) for yy, xx in ((1 - y, 1 - x), (y, 1 - x), (1 - y, x)) for cc in (c, 1 - c)]
    user = (x, 2 * (1 - x) + c)
    rows, cols = a_v.shape
    half, quarter = rows // 2, rows // 4
    sub = half // SUBS
    feat_in, classes = feat.shape[0], grad.shape[0]
    my_cols, peer_cols = c * rows, (1 - c) * rows

    def rcopy(src, dst, send, recv, dev):
        return pltpu.make_async_remote_copy(
            src_ref=src, dst_ref=dst, send_sem=send_sem.at[send], recv_sem=recv_sem.at[recv],
            device_id=dev, device_id_type=MESH)

    def wait_recv(dst, recv):
        rcopy(dst, dst, 0, recv, peer).wait_recv()

    def wait_send(src, send):
        rcopy(src, src, send, 0, peer).wait_send()

    side = jnp.where(diag, 0, 1)
    hs_loads = [pltpu.make_async_copy(feat.at[:, ds((2 * w + side) * quarter, quarter)],
                                      hs.at[:, pl.ds(w * quarter, quarter)], l_sem.at[4 + w]) for w in range(2)]
    h_load = pltpu.make_async_copy(feat, ht.at[:, ds(my_cols, rows)], l_sem.at[3])
    for load in hs_loads:
        load.start()

    @pl.when(diag)
    def _():
        h_load.start()

    g_load = pltpu.make_async_copy(grad, g_v, l_sem.at[0])
    w1_load = pltpu.make_async_copy(w_one, w1_v, l_sem.at[1])
    w2_load = pltpu.make_async_copy(w_two, w2_v, l_sem.at[2])
    own0, other0 = y * half, (1 - y) * half
    a_rows = [ds(other0, quarter), ds(other0 + quarter, quarter), ds(own0, quarter), ds(own0 + quarter, quarter)]
    a_loads = []
    for i, start in enumerate((other0, other0 + quarter, own0, own0 + quarter)):
        for j in range(2):
            rs = ds(start + j * sub, sub)
            a_loads.append(pltpu.make_async_copy(adj.at[rs], a_v.at[rs], a_sem.at[i]))
    for load in a_loads[:4]:
        load.start()

    def wait_a(i):
        pltpu.make_async_copy(adj.at[a_rows[i]], a_v.at[a_rows[i]], a_sem.at[i]).wait()

    barrier = pltpu.get_barrier_semaphore()
    for dev in (peer, *far):
        pl.semaphore_signal(barrier, inc=1, device_id=dev, device_id_type=MESH)
    pl.semaphore_wait(barrier, 7)

    def h_piece(k):
        return ht.at[:, ds(my_cols + k * quarter, quarter)]

    for w in range(2):
        hs_loads[w].wait()
        rcopy(hs.at[:, pl.ds(w * quarter, quarter)], h_piece(2 * w + side), H_S, H_R + w, user).start()

    for load in a_loads[4:]:
        load.start()
    for load in (g_load, w1_load, w2_load):
        load.start()
    def h_wave(w, start):
        return ht.at[:, ds(start + w * half, half)]

    h_fwd = [rcopy(h_wave(w, my_cols), h_wave(w, my_cols), HT_S, HT_R + w, peer) for w in range(2)]

    @pl.when(diag)
    def _():
        h_load.wait()
        for w in range(2):
            h_fwd[w].start()

    x1_y = []

    def add_x1(rs, cs, first=False):
        part = dot(ht[:, cs], a_v[rs, cs], NT)
        x1p[:, rs] = part if first else x1p[:, rs] + part

    for j in range(SUBS):
        x1_y.append(rcopy(x1p.at[:, ds(other0 + j * sub, sub)], x1_in.at[:, pl.ds(j * sub, sub)], X1Y_S, X1Y_R + j, yn))

    def send_x1(subs, role):
        @pl.when(role)
        def _():
            for j in subs:
                x1_y[j].start()

    def forward_h(w):
        @pl.when(off)
        def _():
            wait_recv(h_wave(w, my_cols), H_R + w)
            h_fwd[w].start()

    waves = [(ds(my_cols + w * half, half), ds(peer_cols + w * half, half)) for w in range(2)]
    def make_dy(role):
        @pl.when(role)
        def _():
            g_load.wait()
            w2_load.wait()
            gbt[...] = g_v[...].astype(BF16)
            dyt[...] = dot(w2_v[...], gbt[...], TN).astype(BF16)

    make_dy(off)
    forward_h(0)
    for i in range(2):
        wait_a(i)
        add_x1(a_rows[i], waves[0][0], True)
    h_fwd[0].wait_recv()
    for i in range(2):
        add_x1(a_rows[i], waves[0][1])
    forward_h(1)
    add_x1(a_rows[0], waves[1][0])
    h_fwd[1].wait_recv()
    for j in range(2):
        add_x1(ds(other0 + j * sub, sub), waves[1][1])
        send_x1((j,), off)
    add_x1(a_rows[1], waves[1][0])
    add_x1(a_rows[1], waves[1][1])
    send_x1(range(SUBS), diag)
    send_x1((2, 3), off)
    for i in range(2, 4):
        wait_a(i)
        x1p[:, a_rows[i]] = dot(ht[...], a_v[a_rows[i], :], NT)

    dz_d2d = []

    def backward(start):
        cs = ds(start, half)
        dzp[:, cs] = dot(dyt[...], a_v[:, cs], NN)

    def mine(ref, h, i):
        return ref.at[:, ds(my_cols + h * half + i * sub, sub)]

    x1_fwd = {(h, i): rcopy(mine(x1t, hv, i), mine(x1t, hv, i), X1D_S, X1D_R + i, peer)
              for h, hv in ((0, y), (1, 1 - y)) for i in range(SUBS)}
    x1_user, x1_col = [], []

    for i in range(SUBS):
        piece = x1s.at[:, pl.ds(i * sub, sub)]
        x1_user.append(rcopy(piece, mine(x1t, y, i), X1U_S, X1G_R + 4 * y + i, user))
        x1_col.append(rcopy(piece, mine(x1t, y, i), X1C_S, X1G_R + 4 * y + i, yn))

    def sum_x1(i):
        x1_y[i].wait_recv()
        cs = pl.ds(i * sub, sub)
        act = (x1p[:, ds(own0 + i * sub, sub)] + x1_in[:, cs]).astype(BF16)
        x1s[:, cs] = act
        x1_user[i].start()

        @pl.when(diag)
        def _():
            mine(x1t, y, i)[...] = act
            x1_fwd[0, i].start()

        @pl.when(off)
        def _():
            x1_col[i].start()

    make_dy(diag)
    for i in range(2):
        backward(peer_cols + i * half)
        dz_d2d.append(rcopy(dzp.at[:, ds(peer_cols + i * half, half)], dz_in.at[:, pl.ds(i * half, half)], DZD_S, DZD_R, peer))
        dz_d2d[-1].start()
        sum_x1(i)
    backward(my_cols)
    sum_x1(2)
    backward(my_cols + half)
    wait_recv(dz_in, DZD_R)
    dz_s[...] = dzp[:, ds(my_cols + (1 - x) * half, half)] + dz_in[:, ds((1 - x) * half, half)]
    sum_x1(3)
    dz_x_copies = []
    for i in range(SUBS):
        cs = pl.ds(i * sub, sub)
        dz_x_copies.append(rcopy(dz_s.at[:, cs], dz_x.at[:, cs], DZX_S, DZX_R + i // (SUBS - 1), xn))

    def send_dz(role):
        @pl.when(role)
        def _():
            for copy in dz_x_copies:
                copy.start()

    send_dz(off)
    w1_load.wait()

    def hidden(start, size):
        cs = ds(start, size)
        z1t[:, cs] = jnp.maximum(dot(w1_v[...], x1t[:, cs], TN), 0.0).astype(BF16)

    halves = (y * half, (1 - y) * half)

    def own_piece(i):
        @pl.when(off)
        def _():
            wait_recv(mine(x1t, y, i), X1G_R + 4 * y + i)
            x1_fwd[0, i].start()

        wait_recv(mine(x1t, 1 - y, i), X1G_R + 4 * (1 - y) + i)
        x1_fwd[1, i].start()
        for h in halves:
            hidden(my_cols + h + i * sub, sub)

    def peer_piece(i):
        wait_recv(x1t.at[:, pl.ds(0, 2 * sub)], X1D_R + i)
        for h in halves:
            hidden(peer_cols + h + i * sub, sub)

    def part_x2(rs, block, group):
        total = None
        for h in halves:
            cs = ds(block + h + group * quarter, quarter)
            part = dot(z1t[:, cs], a_v[rs, cs], NT)
            total = part if total is None else total + part
        return total

    own_piece(0)
    own_piece(1)
    send_dz(diag)
    peer_piece(0)
    peer_piece(1)
    x2p[:, a_rows[0]] = part_x2(a_rows[0], my_cols, 0) + part_x2(a_rows[0], peer_cols, 0)
    own_piece(2)
    own_piece(3)
    peer_piece(2)
    x2p[:, a_rows[0]] += part_x2(a_rows[0], my_cols, 1)
    peer_piece(3)
    x2_y = []
    for j in range(SUBS):
        rs = ds(other0 + j * sub, sub)
        if j < 2:
            x2p[:, rs] += part_x2(rs, peer_cols, 1)
        if j == 2:
            x2p[:, a_rows[1]] = dot(z1t[...], a_v[a_rows[1], :], NT)
        x2_y.append(rcopy(x2p.at[:, rs], x2_in.at[:, pl.ds(j * sub, sub)], X2Y_S, X2Y_R + j // (SUBS - 1), yn))
        x2_y[-1].start()
    for rs in a_rows[2:]:
        x2p[:, rs] = dot(z1t[...], a_v[rs, :], NT)

    dw1 = None
    for i in range(SUBS):
        if i == 0:
            wait_recv(dz_x.at[:, pl.ds(0, half - sub)], DZX_R)
        if i == SUBS - 1:
            wait_recv(dz_x.at[:, pl.ds(0, sub)], DZX_R + 1)
        cs = ds(my_cols + x * half + i * sub, sub)
        d_hidden = (dzp[:, cs] + dz_in[:, ds(x * half + i * sub, sub)]) + dz_x[:, pl.ds(i * sub, sub)]
        d_pre = jnp.where(z1t[:, cs].astype(F32) > 0.0, d_hidden, 0.0).astype(BF16)
        part = dot(x1t[:, cs], d_pre, NT)
        dw1 = part if dw1 is None else dw1 + part
    one_p[pl.ds(0, feat_in)] = dw1
    one_p[pl.ds(feat_in, one_p.shape[0] - feat_in)] = jnp.zeros((one_p.shape[0] - feat_in, one_p.shape[1]), F32)

    n_one = one_p.shape[0] // 2
    one_a = rcopy(one_p.at[ds((1 - c) * n_one, n_one, 8)], one_in, ONE_S, ONE_R, peer)
    one_a.start()
    one_a.wait_recv()
    one_s[...] = one_p[ds(c * n_one, n_one, 8)] + one_in[...]
    one_b = rcopy(one_s, one_x, ONE_S + 1, ONE_R + 1, xn)
    one_b.start()
    one_c = rcopy(one_sx, one_y, ONE_S + 2, ONE_R + 2, yn)

    def send_one_y(role):
        @pl.when(role)
        def _():
            one_b.wait_recv()
            one_sx[...] = one_s[...] + one_x[...]
            one_c.start()

    send_one_y(off)

    dw2 = None
    for i in range(SUBS):
        if i == 0:
            wait_recv(x2_in.at[:, pl.ds(0, half - sub)], X2Y_R)
        if i == SUBS - 1:
            wait_recv(x2_in.at[:, pl.ds(0, sub)], X2Y_R + 1)
        rs = ds(own0 + i * sub, sub)
        act = (x2p[:, rs] + x2_in[:, pl.ds(i * sub, sub)]).astype(BF16)
        part = dot(gbt[:, rs], act, NT)
        dw2 = part if dw2 is None else dw2 + part
    two_p[pl.ds(0, classes)] = dw2
    two_p[pl.ds(classes, two_p.shape[0] - classes)] = jnp.zeros((two_p.shape[0] - classes, two_p.shape[1]), F32)

    n_two = two_p.shape[0] // 2
    me = 2 * (2 * x + y) + c
    two_mine, two_peer = ds(c * n_two, n_two, 8), ds((1 - c) * n_two, n_two, 8)
    for k, dev in enumerate((*far, peer)):
        rows_k = two_mine if k < 6 and k % 2 == 0 else two_peer
        rcopy(two_p.at[rows_k], two_all.at[me], TWO_S, TWO_R, dev).start()
    two_all[me] = two_p[two_mine]
    send_one_y(diag)
    one_c.wait_recv()
    one_mine = ds(c * n_one, n_one, 8)
    one_tot[one_mine] = one_sx[...] + one_y[...]
    one_d = rcopy(one_tot.at[one_mine], one_tot.at[one_mine], ONE_S + 3, ONE_R + 3, peer)
    one_d.start()
    wait_recv(two_all.at[pl.ds(0, 7)], TWO_R)
    pairs = [two_all[2 * k] + two_all[2 * k + 1] for k in range(4)]
    two_tot[two_mine] = (pairs[0] + pairs[1]) + (pairs[2] + pairs[3])
    two_c = rcopy(two_tot.at[two_mine], two_tot.at[two_mine], TWO_S + 1, TWO_R + 1, peer)
    two_c.start()
    one_d.wait_recv()
    dw1_store = pltpu.make_async_copy(one_tot, dw1_out, l_sem.at[6])
    dw1_store.start()
    two_c.wait_recv()
    dw2_store = pltpu.make_async_copy(two_tot, dw2t_out, l_sem.at[7])
    dw2_store.start()

    wait_send(hs, H_S)
    wait_send(ht.at[:, pl.ds(0, rows)], HT_S)
    wait_send(x1_in, X1Y_S)
    wait_send(x1s, X1U_S)

    @pl.when(off)
    def _():
        wait_send(x1s, X1C_S)

    wait_send(x1t.at[:, pl.ds(0, rows)], X1D_S)
    wait_send(dz_in, DZD_S)
    wait_send(dz_s, DZX_S)
    wait_send(x2_in, X2Y_S)
    for copy in (one_a, one_b, one_c, one_d, two_c):
        copy.wait_send()
    wait_send(two_all.at[pl.ds(0, 7)], TWO_S)
    dw1_store.wait()
    dw2_store.wait()


def finish_kernel(one, two, dw1, dw2t):
    dw1[...] = one[pl.ds(0, dw1.shape[0])]
    dw2t[...] = two[pl.ds(0, dw2t.shape[0])]


def solution(mesh):
    def local_step(adj, feat, w_one, w_two, grad):
        rows, cols = adj.shape
        feat_in, hidden = w_one.shape
        classes = w_two.shape[1]
        half = rows // 2
        fpad, cpad = -(-feat_in // 16) * 16, -(-classes // 16) * 16
        vmem = pltpu.VMEM
        one_half = vmem((fpad // 2, hidden), F32)
        dw1, dw2t = pl.pallas_call(
            gcn_kernel,
            out_shape=(jax.ShapeDtypeStruct((fpad, hidden), F32), jax.ShapeDtypeStruct((cpad, hidden), F32)),
            in_specs=[pl.BlockSpec(memory_space=pltpu.HBM)] * 5,
            out_specs=(pl.BlockSpec(memory_space=pltpu.HBM), pl.BlockSpec(memory_space=pltpu.HBM)),
            scratch_shapes=[
                vmem((rows, cols), BF16),
                vmem((feat_in, cols), BF16),
                vmem((feat_in, half), BF16),
                vmem((classes, rows), F32),
                vmem((feat_in, hidden), BF16),
                vmem((classes, hidden), BF16),
                vmem((classes, rows), BF16),
                vmem((hidden, rows), BF16),
                vmem((hidden, cols), F32),
                vmem((hidden, rows), F32),
                vmem((hidden, half), F32),
                vmem((hidden, half), F32),
                vmem((feat_in, rows), F32),
                vmem((feat_in, half), F32),
                vmem((feat_in, half), BF16),
                vmem((feat_in, cols), BF16),
                vmem((hidden, cols), BF16),
                vmem((hidden, rows), F32),
                vmem((hidden, half), F32),
                vmem((fpad, hidden), F32),
                *[one_half] * 5,
                vmem((fpad, hidden), F32),
                vmem((cpad, hidden), F32),
                vmem((8, cpad // 2, hidden), F32),
                vmem((cpad, hidden), F32),
                pltpu.SemaphoreType.DMA((4,)),
                pltpu.SemaphoreType.DMA((8,)),
                pltpu.SemaphoreType.DMA((N_SEND,)),
                pltpu.SemaphoreType.DMA((N_RECV,)),
            ],
            compiler_params=pltpu.CompilerParams(
                collective_id=0, has_side_effects=True, vmem_limit_bytes=60 * 1024 * 1024),
        )(adj, feat.T, w_one, w_two.T, grad.T)
        dw1, dw2t = pl.pallas_call(
            finish_kernel,
            out_shape=(jax.ShapeDtypeStruct((feat_in, hidden), F32), jax.ShapeDtypeStruct((classes, hidden), F32)),
            in_specs=[pl.BlockSpec(memory_space=vmem)] * 2,
            out_specs=(pl.BlockSpec(memory_space=vmem),) * 2,
        )(dw1, dw2t)
        return dw1, dw2t.T

    return jax.shard_map(
        local_step, mesh=mesh,
        in_specs=(P("rows", "rep"), P("rows", None), P(), P(), P("rows", None)),
        out_specs=(P(), P()), check_vma=False)
```
